32 devices in a mesh: chord: 4 (over z), span: 8 (over y, x, core).
Axes of the slice: x: 2, y: 2, z: 4, core: 2. Of those that a mesh axis runs over, the one named last changes fastest.
Arguments:
- state: float32 [5, 125, 16, 16, 128], P(None, None, 'chord', 'span'), may hold values from -10 to 10
Outputs:
- residual: float32 [5, 125, 16, 16, 128], P(None, None, 'chord', 'span')
- viscosity: float32 [125, 16, 16, 128], P(None, 'chord', 'span')
The draws below stay inside these ranges and needn't reach their ends.
All inputs are finite; a program needn't handle non-finite values.
Results may differ from the reference program's by a relative error of at most 0.0001.
Values sent between devices are 32-bit elements; how exact they have to be, the bound alone decides.
A program may use at most 128 MiB of HBM per device.

```python
import math
import jax
import jax.numpy as jnp
import numpy as np
from jax import lax

NVAR = 5
NPTS = 125
NORMAL_ELEMENTS = 128
CHORD_ELEMENTS = 16
SPAN_ELEMENTS = 16


def draw_state(key, part):
    element_lattice = (CHORD_ELEMENTS, SPAN_ELEMENTS, NORMAL_ELEMENTS)
    variable = jnp.arange(NVAR).reshape(NVAR, 1, 1, 1, 1)
    level_base = jax.random.normal(jax.random.fold_in(key, 1), (NVAR, 1) + element_lattice, jnp.float32)
    density_base = jax.random.uniform(jax.random.fold_in(key, 2), (NVAR, 1) + element_lattice, jnp.float32, 0.5, 1.5)
    base = jnp.where(variable == 0, density_base, level_base)
    log_amp = jax.random.uniform(jax.random.fold_in(key, 3), (NVAR, 1) + element_lattice, jnp.float32, math.log(0.001), math.log(1.0))
    noise = jax.random.normal(jax.random.fold_in(key, 4), (NVAR, NPTS) + element_lattice, jnp.float32)
    return jnp.clip(base + jnp.exp(log_amp) * noise, -10.0, 10.0)


def setup_inputs(seed: int = 0) -> dict:
    key_of = jax.random.split(jax.random.key(seed), 2)
    return {
        "state": draw_state(jax.random.fold_in(key_of[1], 71), 0),
    }


EPS_SCALE = 0.01
SENSOR_CENTRE = -3.0
SENSOR_WIDTH = 1.5
RATIO_FLOOR = 1e-06
ENERGY_EPS = 1e-06
GAUSS_NODES = [-0.906179845938664, -0.5384693101056831, 0.0, 0.5384693101056831, 0.906179845938664]
GAUSS_WEIGHTS = [0.2369268850561891, 0.4786286704993665, 0.5688888888888889, 0.4786286704993665, 0.2369268850561891]

def legendre_values(points):
    values = [np.ones(points.shape), np.array(points)]
    for order in range(1, 5):
        values.append(((2 * order + 1) * points * values[order] - order * values[order - 1]) / (order + 1))
    return values

def line_tables():
    line_nodes = np.array(GAUSS_NODES)
    quadrature_weights = np.array(GAUSS_WEIGHTS)
    barycentric = np.array([1.0 / np.prod([line_nodes[j] - line_nodes[k] for k in range(5) if k != j]) for j in range(5)])
    derivative = np.zeros((5, 5))
    for i in range(5):
        for j in range(5):
            if i != j:
                derivative[i, j] = barycentric[j] / barycentric[i] / (line_nodes[i] - line_nodes[j])
        derivative[i, i] = -np.sum(derivative[i])
    left_values = np.ones(5)
    right_values = np.ones(5)
    for j in range(5):
        for k in range(5):
            if k != j:
                left_values[j] *= (-1.0 - line_nodes[k]) / (line_nodes[j] - line_nodes[k])
                right_values[j] *= (1.0 - line_nodes[k]) / (line_nodes[j] - line_nodes[k])
    legendre = legendre_values(line_nodes)
    fourth_slope = 7.0 * legendre[3] + 3.0 * legendre[1]
    fifth_slope = 9.0 * legendre[4] + 5.0 * legendre[2] + legendre[0]
    left_corr = 0.5 * (fourth_slope - fifth_slope)
    right_corr = 0.5 * (fourth_slope + fifth_slope)
    modal = np.zeros((5, 5))
    for k in range(5):
        modal[k, :] = quadrature_weights * math.sqrt((2 * k + 1) / 2.0) * legendre[k]
    return (line_nodes, derivative, left_values, right_values, left_corr, right_corr, modal)

def along_axis(operator_matrix, axis):
    factors = [np.eye(5), np.eye(5), np.eye(5)]
    factors[axis] = operator_matrix
    return np.kron(np.kron(factors[0], factors[1]), factors[2])

def build_tables():
    line_nodes, derivative, left_values, right_values, left_corr, right_corr, modal = line_tables()
    operators = []
    for axis in range(3):
        group = (along_axis(derivative, axis), along_axis(left_values[None, :], axis), along_axis(right_values[None, :], axis), along_axis(left_corr[:, None], axis), along_axis(right_corr[:, None], axis))
        operators.append(tuple((jnp.asarray(entry, dtype=jnp.float32) for entry in group)))
    modal_3d = jnp.asarray(np.kron(np.kron(modal, modal), modal), dtype=jnp.float32)
    point_index = np.arange(125)
    high_np = np.where((point_index // 25 == 4) | (point_index // 5 % 5 == 4) | (point_index % 5 == 4), 1.0, 0.0)
    high_mask = jnp.asarray(high_np, dtype=jnp.float32)
    halves = [(1.0 - line_nodes) / 2.0, (1.0 + line_nodes) / 2.0]
    trilinear_np = np.zeros((125, 8))
    for corner in range(8):
        trilinear_np[:, corner] = np.kron(np.kron(halves[corner // 4], halves[corner // 2 % 2]), halves[corner % 2])
    trilinear = jnp.asarray(trilinear_np, dtype=jnp.float32)
    return (operators, modal_3d, high_mask, trilinear)

def single_points(operator_matrix, field):
    return jnp.einsum('qp,pxyz->qxyz', operator_matrix, field, precision=lax.Precision.HIGHEST)

def sensor_viscosity(density, modal_3d, high_mask):
    coeffs = single_points(modal_3d, density)
    energy = coeffs * coeffs
    high_part = lax.optimization_barrier(jnp.sum(energy * high_mask[:, None, None, None], axis=0))
    total = lax.optimization_barrier(jnp.sum(energy, axis=0)) + ENERGY_EPS
    level = jnp.log10(jnp.maximum(high_part / total, RATIO_FLOOR))
    ramp = jnp.clip((level - SENSOR_CENTRE) / SENSOR_WIDTH, -1.0, 1.0)
    return EPS_SCALE * 0.5 * (1.0 + jnp.sin(0.5 * math.pi * ramp))

def boundary_masks(length, dim, rank, is_first, is_last):
    shape = [1] * rank
    shape[dim] = length
    place = lax.broadcasted_iota(jnp.int32, tuple(shape), dim)
    lower_open = jnp.logical_or(place > 0, jnp.logical_not(is_first))
    upper_open = jnp.logical_or(place < length - 1, jnp.logical_not(is_last))
    return (lower_open.astype(jnp.float32), upper_open.astype(jnp.float32))

def variable_residual(field, viscosity, operators):
    total = jnp.zeros_like(field)
    for axis in range(3):
        derivative, to_left, to_right, lift_left, lift_right = operators[axis]
        dim = axis + 1
        closed = axis != 1
        lower_open, upper_open = boundary_masks(field.shape[dim], dim, 4, closed, closed)
        left_tr = single_points(to_left, field)
        right_tr = single_points(to_right, field)
        prev_right = jnp.roll(right_tr, 1, axis=dim)
        following_left = jnp.roll(left_tr, -1, axis=dim)
        gradient = single_points(derivative, field) + single_points(lift_left, 0.5 * (prev_right - left_tr) * lower_open) + single_points(lift_right, 0.5 * (following_left - right_tr) * upper_open)
        flux = viscosity * gradient
        flux_left = single_points(to_left, flux)
        flux_right = single_points(to_right, flux)
        flux_prev = jnp.roll(flux_right, 1, axis=dim)
        flux_next = jnp.roll(flux_left, -1, axis=dim)
        total = total + single_points(derivative, flux) + single_points(lift_left, 0.5 * (flux_prev + flux_left) * lower_open - flux_left) + single_points(lift_right, 0.5 * (flux_next + flux_right) * upper_open - flux_right)
    return total

def reference(state):
    operators, modal_3d, high_mask, trilinear = build_tables()
    element_eps = sensor_viscosity(state[0], modal_3d, high_mask)
    padded = jnp.pad(element_eps, ((1, 1), (0, 0), (1, 1)))
    along_chord = jnp.maximum(padded[:-1], padded[1:])
    along_span = jnp.maximum(along_chord, jnp.roll(along_chord, 1, axis=1))
    vertex = jnp.maximum(along_span[:, :, :-1], along_span[:, :, 1:])
    shifted = jnp.roll(vertex, -1, axis=1)
    chord_count = element_eps.shape[0]
    normal_count = element_eps.shape[2]
    corner_list = []
    for corner in range(8):
        step_x = corner // 4
        step_y = corner // 2 % 2
        step_z = corner % 2
        source = shifted if step_y == 1 else vertex
        corner_list.append(source[step_x:step_x + chord_count, :, step_z:step_z + normal_count])
    corners = jnp.stack(corner_list, axis=0)
    viscosity = jnp.einsum('qc,cxyz->qxyz', trilinear, corners, precision=lax.Precision.HIGHEST)

    def one_variable(field):
        return variable_residual(field, viscosity, operators)
    residual = lax.map(one_variable, state)
    return (residual, viscosity)
```

```python
import functools
import math

import jax
import jax.numpy as jnp
import numpy as np
from jax import lax
from jax.experimental import pallas as pl
from jax.experimental.pallas import tpu as pltpu
from jax.sharding import PartitionSpec as P

EPS_SCALE = 0.01
SENSOR_CENTRE = -3.0
SENSOR_WIDTH = 1.5
RATIO_FLOOR = 1e-06
ENERGY_EPS = 1e-06
GAUSS_NODES = [-0.906179845938664, -0.5384693101056831, 0.0, 0.5384693101056831, 0.906179845938664]
GAUSS_WEIGHTS = [
    0.2369268850561891,
    0.4786286704993665,
    0.5688888888888889,
    0.4786286704993665,
    0.2369268850561891,
]


def legendre_values(points):
    values = [np.ones(points.shape), np.array(points)]
    for order in range(1, 5):
        values.append(
            ((2 * order + 1) * points * values[order] - order * values[order - 1]) / (order + 1)
        )
    return values


def line_tables():
    line_nodes = np.array(GAUSS_NODES)
    quadrature_weights = np.array(GAUSS_WEIGHTS)
    barycentric = np.array(
        [
            1.0 / np.prod([line_nodes[j] - line_nodes[k] for k in range(5) if k != j])
            for j in range(5)
        ]
    )
    derivative = np.zeros((5, 5))
    for i in range(5):
        for j in range(5):
            if i != j:
                derivative[i, j] = barycentric[j] / barycentric[i] / (line_nodes[i] - line_nodes[j])
        derivative[i, i] = -np.sum(derivative[i])
    left_values = np.ones(5)
    right_values = np.ones(5)
    for j in range(5):
        for k in range(5):
            if k != j:
                left_values[j] *= (-1.0 - line_nodes[k]) / (line_nodes[j] - line_nodes[k])
                right_values[j] *= (1.0 - line_nodes[k]) / (line_nodes[j] - line_nodes[k])
    legendre = legendre_values(line_nodes)
    fourth_slope = 7.0 * legendre[3] + 3.0 * legendre[1]
    fifth_slope = 9.0 * legendre[4] + 5.0 * legendre[2] + legendre[0]
    left_corr = 0.5 * (fourth_slope - fifth_slope)
    right_corr = 0.5 * (fourth_slope + fifth_slope)
    modal = np.zeros((5, 5))
    for k in range(5):
        modal[k, :] = quadrature_weights * math.sqrt((2 * k + 1) / 2.0) * legendre[k]
    return (line_nodes, derivative, left_values, right_values, left_corr, right_corr, modal)


NODES, DERIV, LEFT, RIGHT, LIFT_LEFT, LIFT_RIGHT, MODAL = line_tables()
HALF_LEFT = 0.5 * LIFT_LEFT
HALF_RIGHT = 0.5 * LIFT_RIGHT


def fold(u):
    return (u[0] + u[4], u[1] + u[3], u[2], u[0] - u[4], u[1] - u[3])


def traces(parts):
    s0, s1, mid, d0, d1 = parts
    r = [float(x) for x in RIGHT]
    even = 0.5 * (r[0] + r[4]) * s0 + 0.5 * (r[1] + r[3]) * s1 + r[2] * mid
    odd = 0.5 * (r[0] - r[4]) * d0 + 0.5 * (r[1] - r[3]) * d1
    return even - odd, even + odd


def slope(parts, jump_left, jump_right):
    s0, s1, mid, d0, d1 = parts
    h = [float(x) for x in HALF_LEFT]
    diff = jump_left - jump_right
    both = jump_left + jump_right
    even, odd = [], []
    for i in range(3):
        even.append(
            float(0.5 * (DERIV[i, 0] - DERIV[i, 4])) * d0
            + float(0.5 * (DERIV[i, 1] - DERIV[i, 3])) * d1
            + 0.5 * (h[i] + h[4 - i]) * diff
        )
    for i in range(2):
        odd.append(
            float(0.5 * (DERIV[i, 0] + DERIV[i, 4])) * s0
            + float(0.5 * (DERIV[i, 1] + DERIV[i, 3])) * s1
            + float(DERIV[i, 2]) * mid
            + 0.5 * (h[i] - h[4 - i]) * both
        )
    return [even[0] + odd[0], even[1] + odd[1], even[2], even[1] - odd[1], even[0] - odd[0]]


def points(axis, q, j):
    if axis == 0:
        return [25 * i + 5 * q + j for i in range(5)]
    if axis == 1:
        return [25 * q + 5 * i + j for i in range(5)]
    return [25 * q + 5 * j + i for i in range(5)]


def modal_line(u):
    s0, s1, mid, d0, d1 = fold(u)
    out = []
    for k in range(5):
        m = [float(x) for x in MODAL[k]]
        out.append(m[0] * s0 + m[1] * s1 + m[2] * mid if k % 2 == 0 else m[0] * d0 + m[1] * d1)
    return out


def sensor(load, work):
    def first(q, carry):
        for j in range(5):
            pts = points(0, q, j)
            for i, value in zip(pts, modal_line([load(p) for p in pts])):
                work[i] = value
        return carry

    lax.fori_loop(0, 5, first, 0)

    def second(q, carry):
        total, high = carry
        plane = {}
        for c in range(5):
            for b, value in enumerate(modal_line([work[25 * q + 5 * b + c] for b in range(5)])):
                plane[b, c] = value
        low = jnp.zeros_like(total)
        edge = jnp.zeros_like(total)
        for b in range(5):
            line = modal_line([plane[b, c] for c in range(5)])
            squares = [x * x for x in line]
            if b < 4:
                low = low + ((squares[0] + squares[1]) + (squares[2] + squares[3]))
                edge = edge + squares[4]
            else:
                edge = edge + ((squares[0] + squares[1]) + (squares[2] + squares[3])) + squares[4]
        plane_total = low + edge
        return total + plane_total, high + jnp.where(q == 4, plane_total, edge)

    zero = jnp.zeros(work.shape[1:], jnp.float32)
    total, high = lax.fori_loop(0, 5, second, (zero, zero))
    level = jnp.log(jnp.maximum(high / (total + ENERGY_EPS), RATIO_FLOOR)) * (1.0 / math.log(10.0))
    ramp = jnp.clip((level - SENSOR_CENTRE) / SENSOR_WIDTH, -1.0, 1.0)
    return EPS_SCALE * 0.5 * (1.0 + jnp.sin(0.5 * math.pi * ramp))


def rolled(value, shift, axis):
    size = value.shape[axis]
    return pltpu.roll(value, shift % size, axis)


def interpolate(neighbours, nu):
    rows, lanes = nu.shape[1:]
    lane = lax.broadcasted_iota(jnp.int32, (rows, lanes), 1)
    corner = {}
    for x in range(2):
        for y in range(2):
            line = jnp.maximum(
                jnp.maximum(neighbours[x][y], neighbours[x + 1][y]),
                jnp.maximum(neighbours[x][y + 1], neighbours[x + 1][y + 1]),
            )
            before = jnp.where(lane == 0, 0.0, rolled(line, 1, 1))
            after = jnp.where(lane == lanes - 1, 0.0, rolled(line, -1, 1))
            corner[x, y, 0] = jnp.maximum(line, before)
            corner[x, y, 1] = jnp.maximum(line, after)
    lower = [float((1.0 - x) / 2.0) for x in NODES]
    upper = [float((1.0 + x) / 2.0) for x in NODES]
    for a in range(5):
        face = {
            (y, z): lower[a] * corner[0, y, z] + upper[a] * corner[1, y, z]
            for y in range(2)
            for z in range(2)
        }
        for b in range(5):
            edge = [lower[b] * face[0, z] + upper[b] * face[1, z] for z in range(2)]
            for c in range(5):
                nu[25 * a + 5 * b + c] = lower[c] * edge[0] + upper[c] * edge[1]


def row_masks(axis, chords, spans, lanes):
    row = lax.broadcasted_iota(jnp.int32, (chords * spans, lanes), 0)
    if axis == 0:
        return row < spans, row >= (chords - 1) * spans
    place = row % spans
    return place == 0, place == spans - 1


def outer_rows(axis, chords, spans, last):
    if axis == 0:
        return pl.ds((chords - 1) * spans if last else 0, spans)
    return pl.ds(spans - 1 if last else 0, chords, spans)


def trace_kernel(chords, spans, state, eps, c_up, c_down, s_up, s_down, work):
    v = pl.program_id(0)

    @pl.when(v == 0)
    def _():
        eps[...] = sensor(lambda p: state[0, p], work)

    for axis, up, down in ((0, c_up, c_down), (1, s_up, s_down)):

        def body(q, carry):
            for j in range(5):
                left, right = traces(fold([state[0, p] for p in points(axis, q, j)]))
                work[2 * j] = left
                work[2 * j + 1] = right
                down[v, 5 * q + j] = work[2 * j, outer_rows(axis, chords, spans, False)]
                up[v, 5 * q + j] = work[2 * j + 1, outer_rows(axis, chords, spans, True)]
            return carry

        lax.fori_loop(0, 5, body, 0)


def flux_kernel(chords, spans, state, around, nu, c_up, c_down, s_up, s_down, work):
    v = pl.program_id(0)
    lanes = nu.shape[-1]

    @pl.when(v == 0)
    def _():
        interpolate([[around[x, y] for y in range(3)] for x in range(3)], nu)

    for axis, up, down in ((0, c_up, c_down), (1, s_up, s_down)):
        low, high = row_masks(axis, chords, spans, lanes)
        step = spans if axis == 0 else 1
        rows_low = outer_rows(axis, chords, spans, False)
        rows_high = outer_rows(axis, chords, spans, True)

        def body(q, carry):
            for j in range(5):
                pts = points(axis, q, j)
                parts = fold([state[0, p] for p in pts])
                left, right = traces(parts)
                before = jnp.where(low, 0.0, rolled(right, step, 0))
                after = jnp.where(high, 0.0, rolled(left, -step, 0))
                gradient = slope(parts, before - left, after - right)
                flux = [nu[p] * g for p, g in zip(pts, gradient)]
                left, right = traces(fold(flux))
                work[2 * j] = left
                work[2 * j + 1] = right
                down[v, 5 * q + j] = work[2 * j, rows_low]
                up[v, 5 * q + j] = work[2 * j + 1, rows_high]
            return carry

        lax.fori_loop(0, 5, body, 0)

        @pl.when(v == 0)
        def _():
            def weights(q, carry):
                for j in range(5):
                    local = [nu[p] for p in points(axis, q, j)]
                    left = sum(float(LEFT[i] * HALF_LEFT[i]) * local[i] for i in range(5))
                    right = sum(float(RIGHT[i] * HALF_RIGHT[i]) * local[i] for i in range(5))
                    work[2 * j] = left
                    work[2 * j + 1] = right
                    down[pl.num_programs(0), 5 * q + j] = work[2 * j, rows_low]
                    up[pl.num_programs(0), 5 * q + j] = work[2 * j + 1, rows_high]
                return carry

            lax.fori_loop(0, 5, weights, 0)


def residual_kernel(
    chords, spans, state, nu, c_up, c_down, s_up, s_down,
    fc_up, fc_down, fs_up, fs_down, out, ghost, alpha, beta,
):
    v = pl.program_id(0)
    count = pl.num_programs(0)
    rows, lanes = nu.shape[1:]
    lane = lax.broadcasted_iota(jnp.int32, (rows, lanes), 1)
    row = lax.broadcasted_iota(jnp.int32, (rows, lanes), 0)
    place = lax.axis_index("chord")
    closed_low = row < jnp.where(place == 0, spans, 0)
    closed_high = row >= jnp.where(place == lax.axis_size("chord") - 1, rows - spans, rows)

    def normal(q, carry):
        first, last = lane == 0, lane == lanes - 1
        for j in range(5):
            pts = points(2, q, j)
            parts = fold([state[0, p] for p in pts])
            left, right = traces(parts)
            jump_left = jnp.where(first, 0.0, rolled(right, 1, 1) - left)
            jump_right = jnp.where(last, 0.0, rolled(left, -1, 1) - right)
            parts = fold([nu[p] * g for p, g in zip(pts, slope(parts, jump_left, jump_right))])
            left, right = traces(parts)
            jump_left = jnp.where(first, -left, rolled(right, 1, 1)) - left
            jump_right = jnp.where(last, -right, rolled(left, -1, 1)) - right
            for p, value in zip(pts, slope(parts, jump_left, jump_right)):
                out[0, p] = value
        return carry

    lax.fori_loop(0, 5, normal, 0)

    for axis, up, down, f_up, f_down in (
        (0, c_up, c_down, fc_up, fc_down),
        (1, s_up, s_down, fs_up, fs_down),
    ):
        low, high = row_masks(axis, chords, spans, lanes)
        step = spans if axis == 0 else 1
        rows_low = outer_rows(axis, chords, spans, False)
        rows_high = outer_rows(axis, chords, spans, True)

        def gather(q, carry):
            for j in range(5):
                f = 5 * q + j
                ghost[f, rows_low] = up[v, f]
                ghost[f, rows_high] = down[v, f]
                alpha[f, rows_low] = f_up[v, f]
                alpha[f, rows_high] = f_down[v, f]
                beta[f, rows_low] = f_up[count, f]
                beta[f, rows_high] = f_down[count, f]
            return carry

        lax.fori_loop(0, 5, gather, 0)

        def body(q, carry):
            for j in range(5):
                f = 5 * q + j
                pts = points(axis, q, j)
                parts = fold([state[0, p] for p in pts])
                left, right = traces(parts)
                outside = ghost[f]
                before = jnp.where(low, outside, rolled(right, step, 0))
                after = jnp.where(high, outside, rolled(left, -step, 0))
                jump_left = before - left
                jump_right = after - right
                if axis == 0:
                    jump_left = jnp.where(closed_low, 0.0, jump_left)
                    jump_right = jnp.where(closed_high, 0.0, jump_right)
                own_left, own_right = left, right
                flux = [nu[p] * g for p, g in zip(pts, slope(parts, jump_left, jump_right))]
                parts = fold(flux)
                left, right = traces(parts)
                a, b = alpha[f], beta[f]
                before = jnp.where(low, a + b * own_left, rolled(right, step, 0))
                after = jnp.where(high, a + b * own_right, rolled(left, -step, 0))
                if axis == 0:
                    before = jnp.where(closed_low, -left, before)
                    after = jnp.where(closed_high, -right, after)
                for p, value in zip(pts, slope(parts, before - left, after - right)):
                    out[0, p] += value
            return carry

        lax.fori_loop(0, 5, body, 0)


def along(block, axis, by):
    devices = lax.axis_size(axis)
    route = [(i, i + by) for i in range(devices)]
    if axis == "span":
        route = [(i, j % devices) for i, j in route]
    else:
        route = [(i, j) for i, j in route if 0 <= j < devices]
    return lax.ppermute(block, axis, route)


def grown(eps):
    for axis, dim in (("span", 1), ("chord", 0)):
        length = eps.shape[dim]
        before = along(lax.slice_in_dim(eps, length - 1, length, axis=dim), axis, 1)
        after = along(lax.slice_in_dim(eps, 0, 1, axis=dim), axis, -1)
        eps = jnp.concatenate([before, eps, after], axis=dim)
    return eps


def shards(state):
    count, npts, chords, spans, lanes = state.shape
    rows = chords * spans
    flat = state.reshape(count, npts, rows, lanes)
    f32 = jnp.float32
    per_variable = pl.BlockSpec((1, npts, rows, lanes), lambda v: (v, 0, 0, 0))

    def whole(*shape):
        return pl.BlockSpec(shape, lambda v: (0,) * len(shape))

    def messages(n):
        shapes = [(n, 25, spans, lanes)] * 2 + [(n, 25, chords, lanes)] * 2
        return [whole(*s) for s in shapes], [jax.ShapeDtypeStruct(s, f32) for s in shapes]

    specs, shapes = messages(count)
    f_specs, f_shapes = messages(count + 1)
    eps, *traced = pl.pallas_call(
        functools.partial(trace_kernel, chords, spans),
        grid=(count,),
        in_specs=[per_variable],
        out_specs=[whole(rows, lanes)] + specs,
        out_shape=[jax.ShapeDtypeStruct((rows, lanes), f32)] + shapes,
        scratch_shapes=[pltpu.VMEM((npts, rows, lanes), f32)],
    )(flat)
    steps = (("chord", 1), ("chord", -1), ("span", 1), ("span", -1))
    wide = grown(eps.reshape(chords, spans, lanes))
    ghosts = [along(m, axis, by) for m, (axis, by) in zip(traced, steps)]
    around = jnp.stack(
        [wide[x : x + chords, y : y + spans] for x in range(3) for y in range(3)]
    ).reshape(3, 3, rows, lanes)
    nu, *fluxes = pl.pallas_call(
        functools.partial(flux_kernel, chords, spans),
        grid=(count,),
        in_specs=[per_variable, whole(3, 3, rows, lanes)],
        out_specs=[whole(npts, rows, lanes)] + f_specs,
        out_shape=[jax.ShapeDtypeStruct((npts, rows, lanes), f32)] + f_shapes,
        scratch_shapes=[pltpu.VMEM((10, rows, lanes), f32)],
    )(flat, around)
    flux_ghosts = [along(m, axis, by) for m, (axis, by) in zip(fluxes, steps)]
    residual = pl.pallas_call(
        functools.partial(residual_kernel, chords, spans),
        grid=(count,),
        in_specs=[per_variable, whole(npts, rows, lanes)] + specs + f_specs,
        out_specs=per_variable,
        out_shape=jax.ShapeDtypeStruct(flat.shape, f32),
        scratch_shapes=[pltpu.VMEM((25, rows, lanes), f32)] * 3,
    )(flat, nu, *ghosts, *flux_ghosts)
    return residual.reshape(state.shape), nu.reshape(npts, chords, spans, lanes)


def solution(mesh):
    in_specs = (P(None, None, "chord", "span", None),)
    out_specs = (P(None, None, "chord", "span", None), P(None, "chord", "span", None))
    return jax.shard_map(shards, mesh=mesh, in_specs=in_specs, out_specs=out_specs, check_vma=False)
```

```python
import functools
import math

import jax
import jax.numpy as jnp
import numpy as np
from jax import lax
from jax.experimental import pallas as pl
from jax.experimental.pallas import tpu as pltpu
from jax.sharding import PartitionSpec as P

EPS_SCALE = 0.01
SENSOR_CENTRE = -3.0
SENSOR_WIDTH = 1.5
RATIO_FLOOR = 1e-06
ENERGY_EPS = 1e-06
GAUSS_NODES = [-0.906179845938664, -0.5384693101056831, 0.0, 0.5384693101056831, 0.906179845938664]
GAUSS_WEIGHTS = [
    0.2369268850561891,
    0.4786286704993665,
    0.5688888888888889,
    0.4786286704993665,
    0.2369268850561891,
]


def legendre_values(points):
    values = [np.ones(points.shape), np.array(points)]
    for order in range(1, 5):
        values.append(
            ((2 * order + 1) * points * values[order] - order * values[order - 1]) / (order + 1)
        )
    return values


def line_tables():
    line_nodes = np.array(GAUSS_NODES)
    quadrature_weights = np.array(GAUSS_WEIGHTS)
    barycentric = np.array(
        [
            1.0 / np.prod([line_nodes[j] - line_nodes[k] for k in range(5) if k != j])
            for j in range(5)
        ]
    )
    derivative = np.zeros((5, 5))
    for i in range(5):
        for j in range(5):
            if i != j:
                derivative[i, j] = barycentric[j] / barycentric[i] / (line_nodes[i] - line_nodes[j])
        derivative[i, i] = -np.sum(derivative[i])
    left_values = np.ones(5)
    right_values = np.ones(5)
    for j in range(5):
        for k in range(5):
            if k != j:
                left_values[j] *= (-1.0 - line_nodes[k]) / (line_nodes[j] - line_nodes[k])
                right_values[j] *= (1.0 - line_nodes[k]) / (line_nodes[j] - line_nodes[k])
    legendre = legendre_values(line_nodes)
    fourth_slope = 7.0 * legendre[3] + 3.0 * legendre[1]
    fifth_slope = 9.0 * legendre[4] + 5.0 * legendre[2] + legendre[0]
    left_corr = 0.5 * (fourth_slope - fifth_slope)
    right_corr = 0.5 * (fourth_slope + fifth_slope)
    modal = np.zeros((5, 5))
    for k in range(5):
        modal[k, :] = quadrature_weights * math.sqrt((2 * k + 1) / 2.0) * legendre[k]
    return (line_nodes, derivative, left_values, right_values, left_corr, right_corr, modal)


NODES, DERIV, LEFT, RIGHT, LIFT_LEFT, LIFT_RIGHT, MODAL = line_tables()
HALF_LEFT = 0.5 * LIFT_LEFT
HALF_RIGHT = 0.5 * LIFT_RIGHT


def fold(u):
    return (u[0] + u[4], u[1] + u[3], u[2], u[0] - u[4], u[1] - u[3])


def traces(parts):
    s0, s1, mid, d0, d1 = parts
    r = [float(x) for x in RIGHT]
    even = 0.5 * (r[0] + r[4]) * s0 + 0.5 * (r[1] + r[3]) * s1 + r[2] * mid
    odd = 0.5 * (r[0] - r[4]) * d0 + 0.5 * (r[1] - r[3]) * d1
    return even - odd, even + odd


def slope(parts, jump_left, jump_right):
    s0, s1, mid, d0, d1 = parts
    h = [float(x) for x in HALF_LEFT]
    diff = jump_left - jump_right
    both = jump_left + jump_right
    even, odd = [], []
    for i in range(3):
        even.append(
            float(0.5 * (DERIV[i, 0] - DERIV[i, 4])) * d0
            + float(0.5 * (DERIV[i, 1] - DERIV[i, 3])) * d1
            + 0.5 * (h[i] + h[4 - i]) * diff
        )
    for i in range(2):
        odd.append(
            float(0.5 * (DERIV[i, 0] + DERIV[i, 4])) * s0
            + float(0.5 * (DERIV[i, 1] + DERIV[i, 3])) * s1
            + float(DERIV[i, 2]) * mid
            + 0.5 * (h[i] - h[4 - i]) * both
        )
    return [even[0] + odd[0], even[1] + odd[1], even[2], even[1] - odd[1], even[0] - odd[0]]


def points(axis, q, j):
    if axis == 0:
        return [25 * i + 5 * q + j for i in range(5)]
    if axis == 1:
        return [25 * q + 5 * i + j for i in range(5)]
    return [25 * q + 5 * j + i for i in range(5)]


def modal_line(u):
    s0, s1, mid, d0, d1 = fold(u)
    out = []
    for k in range(5):
        m = [float(x) for x in MODAL[k]]
        out.append(m[0] * s0 + m[1] * s1 + m[2] * mid if k % 2 == 0 else m[0] * d0 + m[1] * d1)
    return out


def sensor(load, work):
    def first(q, carry):
        for j in range(5):
            pts = points(0, q, j)
            for i, value in zip(pts, modal_line([load(p) for p in pts])):
                work[i] = value
        return carry

    lax.fori_loop(0, 5, first, 0)

    def second(q, carry):
        total, high = carry
        plane = {}
        for c in range(5):
            for b, value in enumerate(modal_line([work[25 * q + 5 * b + c] for b in range(5)])):
                plane[b, c] = value
        low = jnp.zeros_like(total)
        edge = jnp.zeros_like(total)
        for b in range(5):
            line = modal_line([plane[b, c] for c in range(5)])
            squares = [x * x for x in line]
            if b < 4:
                low = low + ((squares[0] + squares[1]) + (squares[2] + squares[3]))
                edge = edge + squares[4]
            else:
                edge = edge + ((squares[0] + squares[1]) + (squares[2] + squares[3])) + squares[4]
        plane_total = low + edge
        return total + plane_total, high + jnp.where(q == 4, plane_total, edge)

    zero = jnp.zeros(work.shape[1:], jnp.float32)
    total, high = lax.fori_loop(0, 5, second, (zero, zero))
    level = jnp.log(jnp.maximum(high / (total + ENERGY_EPS), RATIO_FLOOR)) * (1.0 / math.log(10.0))
    ramp = jnp.clip((level - SENSOR_CENTRE) / SENSOR_WIDTH, -1.0, 1.0)
    return EPS_SCALE * 0.5 * (1.0 + jnp.sin(0.5 * math.pi * ramp))


def rolled(value, shift, axis):
    size = value.shape[axis]
    return pltpu.roll(value, shift % size, axis)


def interpolate(neighbours, nu):
    rows, lanes = nu.shape[1:]
    lane = lax.broadcasted_iota(jnp.int32, (rows, lanes), 1)
    corner = {}
    for x in range(2):
        for y in range(2):
            line = jnp.maximum(
                jnp.maximum(neighbours[x][y], neighbours[x + 1][y]),
                jnp.maximum(neighbours[x][y + 1], neighbours[x + 1][y + 1]),
            )
            before = jnp.where(lane == 0, 0.0, rolled(line, 1, 1))
            after = jnp.where(lane == lanes - 1, 0.0, rolled(line, -1, 1))
            corner[x, y, 0] = jnp.maximum(line, before)
            corner[x, y, 1] = jnp.maximum(line, after)
    lower = [float((1.0 - x) / 2.0) for x in NODES]
    upper = [float((1.0 + x) / 2.0) for x in NODES]
    for a in range(5):
        face = {
            (y, z): lower[a] * corner[0, y, z] + upper[a] * corner[1, y, z]
            for y in range(2)
            for z in range(2)
        }
        for b in range(5):
            edge = [lower[b] * face[0, z] + upper[b] * face[1, z] for z in range(2)]
            for c in range(5):
                nu[25 * a + 5 * b + c] = lower[c] * edge[0] + upper[c] * edge[1]


def row_masks(axis, chords, spans, lanes):
    row = lax.broadcasted_iota(jnp.int32, (chords * spans, lanes), 0)
    if axis == 0:
        return row < spans, row >= (chords - 1) * spans
    place = row % spans
    return place == 0, place == spans - 1


def outer_rows(axis, chords, spans, last):
    if axis == 0:
        return pl.ds((chords - 1) * spans if last else 0, spans)
    return pl.ds(spans - 1 if last else 0, chords, spans)


def store_pair(work, slot, left, right, down, up, index, rows_low, rows_high):
    work[2 * slot] = left
    work[2 * slot + 1] = right
    down[index] = work[2 * slot, rows_low]
    up[index] = work[2 * slot + 1, rows_high]


def local_kernel(sizes, count, chords, spans, *refs):
    state_hbm = refs[0]
    nu, faces_c, faces_s, partial = refs[1:5]
    ghosts = refs[5:9]
    flux_ghosts = refs[9:13]
    (
        state, acc, around, work, eps_out,
        t0, t1, t2, t3, f0, f1, f2, f3,
        load_sem, store_sem, eps_send, eps_recv, send_sem, recv_sem,
    ) = refs[13:]
    sends = ((t0, t1, t2, t3), (f0, f1, f2, f3))
    lands = (ghosts, flux_ghosts)
    rows, lanes = nu.shape[1:]
    chord_size, span_size = sizes
    me_c, me_s = lax.axis_index("chord"), lax.axis_index("span")
    mesh_id = pl.DeviceIdType.MESH

    def load(v):
        return pltpu.make_async_copy(state_hbm.at[v], state.at[v], load_sem.at[v])

    for v in range(count):
        load(v).start()

    def reachable(dx):
        if dx == 0:
            return None
        return me_c + 1 < chord_size if dx == 1 else me_c > 0

    def guarded(cond, run):
        if cond is None:
            run()
        else:
            pl.when(cond)(run)

    def partner(dx, dy):
        return (me_c + dx, lax.rem(me_s + dy + span_size, span_size))

    offsets = [(dx, dy) for dx in (0, -1, 1) for dy in (-1, 0, 1) if (dx, dy) != (0, 0)]
    barrier = pltpu.get_barrier_semaphore()
    for dx, dy in offsets:

        def greet(dx=dx, dy=dy):
            pl.semaphore_signal(barrier, inc=1, device_id=partner(dx, dy), device_id_type=mesh_id)

        guarded(reachable(dx), greet)

    load(0).wait()
    eps = sensor(lambda p: state[0, p], work)
    eps_out[...] = eps
    around[1, 1] = eps
    sides = jnp.where(me_c > 0, 1, 0) + jnp.where(me_c + 1 < chord_size, 1, 0)
    pl.semaphore_wait(barrier, 2 + 3 * sides)

    def eps_copy(dx, dy):
        slot = 3 * (dx + 1) + dy + 1
        return pltpu.make_async_remote_copy(
            src_ref=eps_out, dst_ref=around.at[1 - dx, 1 - dy],
            send_sem=eps_send.at[slot], recv_sem=eps_recv.at[8 - slot],
            device_id=partner(dx, dy), device_id_type=mesh_id,
        )

    for dx, dy in offsets:
        guarded(reachable(dx), lambda dx=dx, dy=dy: eps_copy(dx, dy).start())

    ways = ((1, 0), (-1, 0), (0, 1), (0, -1))

    def message(stage, k, v):
        dx, dy = ways[k]
        return pltpu.make_async_remote_copy(
            src_ref=sends[stage][k].at[v], dst_ref=lands[stage][k].at[v],
            send_sem=send_sem.at[stage, k, v], recv_sem=recv_sem.at[stage, k, v],
            device_id=partner(dx, dy), device_id_type=mesh_id,
        )

    def launch(stage, axis, v):
        for k in (2 * axis, 2 * axis + 1):
            guarded(reachable(ways[k][0]), lambda k=k: message(stage, k, v).start())

    masks = [row_masks(axis, chords, spans, lanes) for axis in range(2)]
    outer = [[outer_rows(axis, chords, spans, last) for last in (False, True)] for axis in range(2)]

    def send_traces(v, carry):
        @pl.when(v > 0)
        def _():
            load(v).wait()

        for axis in (1, 0):
            up, down = sends[0][2 * axis], sends[0][2 * axis + 1]
            faces = (faces_c, faces_s)[axis]

            def body(q, carry):
                for j in range(5):
                    left, right = traces(fold([state[v, p] for p in points(axis, q, j)]))
                    faces[v, 5 * q + j] = jnp.where(masks[axis][0], left, right)
                    store_pair(work, j, left, right, down, up, (v, 5 * q + j), *outer[axis])
                return carry

            lax.fori_loop(0, 5, body, 0)
            launch(0, axis, v)
        return carry

    lax.fori_loop(0, count, send_traces, 0)

    row = lax.broadcasted_iota(jnp.int32, (rows, lanes), 0)
    for dx, dy in offsets:
        guarded(reachable(-dx), lambda dx=dx, dy=dy: eps_copy(dx, dy).wait_recv())

    have_low = jnp.where(me_c > 0, spans, 0)
    have_high = jnp.where(me_c + 1 < chord_size, rows, rows - spans)
    column = []
    for x in range(3):
        mine, left, right = around[x, 1], around[x, 0], around[x, 2]
        column.append([
            jnp.where(masks[1][0], rolled(left, 1 - spans, 0), rolled(mine, 1, 0)),
            mine,
            jnp.where(masks[1][1], rolled(right, spans - 1, 0), rolled(mine, -1, 0)),
        ])
    neighbours = [[], [], []]
    for y in range(3):
        inner = column[1][y]
        below = jnp.where(masks[0][0], rolled(column[0][y], spans, 0), rolled(inner, spans, 0))
        above = jnp.where(masks[0][1], rolled(column[2][y], -spans, 0), rolled(inner, -spans, 0))
        neighbours[0].append(jnp.where(row < spans - have_low, 0.0, below))
        neighbours[1].append(inner)
        neighbours[2].append(jnp.where(row >= have_high, 0.0, above))
    interpolate(neighbours, nu)

    closed_low = row < spans - have_low
    closed_high = row >= have_high

    for axis in (1, 0):
        up, down = sends[1][2 * axis], sends[1][2 * axis + 1]

        def weights(q, carry):
            for j in range(5):
                local = [nu[p] for p in points(axis, q, j)]
                left = sum(float(LEFT[i] * HALF_LEFT[i]) * local[i] for i in range(5))
                right = sum(float(RIGHT[i] * HALF_RIGHT[i]) * local[i] for i in range(5))
                store_pair(work, j, left, right, down, up, (count, 5 * q + j), *outer[axis])
            return carry

        lax.fori_loop(0, 5, weights, 0)
        launch(1, axis, count)

    for axis in (1, 0):

        def variable(v, carry):
            up, down = sends[1][2 * axis], sends[1][2 * axis + 1]
            low, high = masks[axis]
            step = spans if axis == 0 else 1

            def body(q, carry):
                for j in range(5):
                    pts = points(axis, q, j)
                    parts = fold([state[v, p] for p in pts])
                    left, right = traces(parts)
                    jump_left = jnp.where(low, 0.0, rolled(right, step, 0)) - left
                    jump_right = jnp.where(high, 0.0, rolled(left, -step, 0)) - right
                    if axis == 0:
                        jump_left = jnp.where(closed_low, 0.0, jump_left)
                        jump_right = jnp.where(closed_high, 0.0, jump_right)
                    gradient = slope(parts, jump_left, jump_right)
                    parts = fold([nu[p] * g for p, g in zip(pts, gradient)])
                    left, right = traces(parts)
                    store_pair(work, j, left, right, down, up, (v, 5 * q + j), *outer[axis])
                    before = jnp.where(low, 0.0, rolled(right, step, 0))
                    after = jnp.where(high, 0.0, rolled(left, -step, 0))
                    if axis == 0:
                        before = jnp.where(closed_low, -left, before)
                        after = jnp.where(closed_high, -right, after)
                    for p, value in zip(pts, slope(parts, before - left, after - right)):
                        if axis == 1:
                            acc[v, p] = value
                        else:
                            acc[v, p] += value
                return carry

            lax.fori_loop(0, 5, body, 0)
            launch(1, axis, v)
            return carry

        lax.fori_loop(0, count, variable, 0)

    lane = lax.broadcasted_iota(jnp.int32, (rows, lanes), 1)
    first, last = lane == 0, lane == lanes - 1

    def store(v):
        return pltpu.make_async_copy(acc.at[v], partial.at[v], store_sem.at[v])

    def normal(v, carry):
        def body(q, carry):
            for j in range(5):
                pts = points(2, q, j)
                parts = fold([state[v, p] for p in pts])
                left, right = traces(parts)
                jump_left = jnp.where(first, 0.0, rolled(right, 1, 1) - left)
                jump_right = jnp.where(last, 0.0, rolled(left, -1, 1) - right)
                gradient = slope(parts, jump_left, jump_right)
                parts = fold([nu[p] * g for p, g in zip(pts, gradient)])
                left, right = traces(parts)
                jump_left = jnp.where(first, -left, rolled(right, 1, 1)) - left
                jump_right = jnp.where(last, -right, rolled(left, -1, 1)) - right
                for p, value in zip(pts, slope(parts, jump_left, jump_right)):
                    acc[v, p] += value
            return carry

        lax.fori_loop(0, 5, body, 0)
        store(v).start()
        return carry

    lax.fori_loop(0, count, normal, 0)

    for v in range(count):
        store(v).wait()
    for dx, dy in offsets:
        guarded(reachable(dx), lambda dx=dx, dy=dy: eps_copy(dx, dy).wait_send())
    for stage in range(2):
        for k in range(4):
            for v in range(count + stage):
                guarded(reachable(ways[k][0]), lambda k=k, v=v: message(stage, k, v).wait_send())
                guarded(reachable(-ways[k][0]), lambda k=k, v=v: message(stage, k, v).wait_recv())


def ghost_kernel(chords, spans, *refs):
    partial, nu, faces_c, faces_s = refs[:4]
    ghosts, flux_ghosts, weights = refs[4:8], refs[8:12], refs[12:16]
    out, gain, edge, beta, outside, alpha = refs[16:]
    v = pl.program_id(0)
    rows, lanes = nu.shape[1:]
    row = lax.broadcasted_iota(jnp.int32, (rows, lanes), 0)
    place = lax.axis_index("chord")
    closed_low = row < jnp.where(place == 0, spans, 0)
    closed_high = row >= jnp.where(place == lax.axis_size("chord") - 1, rows - spans, rows)

    for axis, faces in ((0, faces_c), (1, faces_s)):
        up, down = ghosts[2 * axis], ghosts[2 * axis + 1]
        f_up, f_down = flux_ghosts[2 * axis], flux_ghosts[2 * axis + 1]
        b_up, b_down = weights[2 * axis], weights[2 * axis + 1]
        low, high = row_masks(axis, chords, spans, lanes)
        step = spans if axis == 0 else 1
        rows_low = outer_rows(axis, chords, spans, False)
        rows_high = outer_rows(axis, chords, spans, True)
        open_low, open_high = low, high
        if axis == 0:
            open_low = low & jnp.logical_not(closed_low)
            open_high = high & jnp.logical_not(closed_high)

        @pl.when(v == 0)
        def _():
            def body(q, carry):
                for j in range(5):
                    f = 5 * q + j
                    beta[axis, f, rows_low] = b_up[0, f]
                    beta[axis, f, rows_high] = b_down[0, f]
                    spread = []
                    for i, p in enumerate(points(axis, q, j)):
                        lift = jnp.where(high, float(HALF_RIGHT[i]), 0.0)
                        lift = jnp.where(low, float(HALF_LEFT[i]), lift)
                        spread.append(nu[p] * lift)
                    parts = fold(spread)
                    left, right = traces(parts)
                    edge[axis, 2 * f] = left
                    edge[axis, 2 * f + 1] = right
                    for i, value in enumerate(slope(parts, -left, -right)):
                        gain[axis, 5 * f + i] = value
                return carry

            lax.fori_loop(0, 5, body, 0)

        def gather(q, carry):
            for j in range(5):
                f = 5 * q + j
                outside[f, rows_low] = up[0, f]
                outside[f, rows_high] = down[0, f]
                alpha[f, rows_low] = f_up[0, f]
                alpha[f, rows_high] = f_down[0, f]
            return carry

        lax.fori_loop(0, 5, gather, 0)

        def body(q, carry):
            for j in range(5):
                f = 5 * q + j
                opened = open_low | open_high
                ghost = jnp.where(opened, outside[f], 0.0)
                flux = jnp.where(opened, alpha[f] + beta[axis, f] * faces[0, f], 0.0)
                before = jnp.where(low, flux, rolled(edge[axis, 2 * f + 1] * ghost, step, 0))
                after = jnp.where(high, flux, rolled(edge[axis, 2 * f] * ghost, -step, 0))
                h = [float(x) for x in HALF_LEFT]
                diff, both = before - after, before + after
                even = [0.5 * (h[i] + h[4 - i]) * diff for i in range(3)]
                odd = [0.5 * (h[i] - h[4 - i]) * both for i in range(2)]
                lifts = [even[0] + odd[0], even[1] + odd[1], even[2], even[1] - odd[1], even[0] - odd[0]]
                for i, p in enumerate(points(axis, q, j)):
                    value = gain[axis, 5 * f + i] * ghost + lifts[i]
                    if axis == 0:
                        out[0, p] = partial[0, p] + value
                    else:
                        out[0, p] += value
            return carry

        lax.fori_loop(0, 5, body, 0)


def shards(state):
    count, npts, chords, spans, lanes = state.shape
    rows = chords * spans
    flat = state.reshape(count, npts, rows, lanes)
    f32 = jnp.float32
    sizes = (lax.axis_size("chord"), lax.axis_size("span"))

    def message(n, k):
        return (n, 25, spans if k < 2 else chords, lanes)

    def full(*shape):
        return jax.ShapeDtypeStruct(shape, f32)

    vmem = pl.BlockSpec(memory_space=pltpu.VMEM)
    hbm = pl.BlockSpec(memory_space=pl.ANY)
    nu, faces_c, faces_s, partial, *moved = pl.pallas_call(
        functools.partial(local_kernel, sizes, count, chords, spans),
        in_specs=[hbm],
        out_specs=[vmem] * 3 + [hbm] * 9,
        out_shape=[full(npts, rows, lanes)] + [full(count, 25, rows, lanes)] * 2
        + [full(count, npts, rows, lanes)]
        + [full(*message(count, k)) for k in range(4)]
        + [full(*message(count + 1, k)) for k in range(4)],
        scratch_shapes=[
            pltpu.VMEM((count, npts, rows, lanes), f32),
            pltpu.VMEM((count, npts, rows, lanes), f32),
            pltpu.VMEM((3, 3, rows, lanes), f32),
            pltpu.VMEM((npts, rows, lanes), f32),
            pltpu.VMEM((rows, lanes), f32),
        ]
        + [pltpu.VMEM(message(count, k), f32) for k in range(4)]
        + [pltpu.VMEM(message(count + 1, k), f32) for k in range(4)]
        + [
            pltpu.SemaphoreType.DMA((count,)),
            pltpu.SemaphoreType.DMA((count,)),
            pltpu.SemaphoreType.DMA((9,)),
            pltpu.SemaphoreType.DMA((9,)),
            pltpu.SemaphoreType.DMA((2, 4, count + 1)),
            pltpu.SemaphoreType.DMA((2, 4, count + 1)),
        ],
        compiler_params=pltpu.CompilerParams(collective_id=0, has_side_effects=True),
    )(flat)

    def block(n, width, fixed=None):
        shape = (1, n, width, lanes)
        return pl.BlockSpec(shape, lambda v: (v if fixed is None else fixed, 0, 0, 0))

    widths = [spans, spans, chords, chords]
    per_variable = block(npts, rows)
    residual = pl.pallas_call(
        functools.partial(ghost_kernel, chords, spans),
        grid=(count,),
        in_specs=[
            per_variable,
            pl.BlockSpec((npts, rows, lanes), lambda v: (0, 0, 0)),
            block(25, rows),
            block(25, rows),
        ]
        + [block(25, w) for w in widths] * 2
        + [block(25, w, count) for w in widths],
        out_specs=per_variable,
        out_shape=full(*flat.shape),
        scratch_shapes=[
            pltpu.VMEM((2, npts, rows, lanes), f32),
            pltpu.VMEM((2, 50, rows, lanes), f32),
            pltpu.VMEM((2, 25, rows, lanes), f32),
            pltpu.VMEM((25, rows, lanes), f32),
            pltpu.VMEM((25, rows, lanes), f32),
        ],
    )(partial, nu, faces_c, faces_s, *moved, *moved[4:])
    return residual.reshape(state.shape), nu.reshape(npts, chords, spans, lanes)


def solution(mesh):
    in_specs = (P(None, None, "chord", "span", None),)
    out_specs = (P(None, None, "chord", "span", None), P(None, "chord", "span", None))
    return jax.shard_map(shards, mesh=mesh, in_specs=in_specs, out_specs=out_specs, check_vma=False)
```

```python
import functools
import math

import jax
import jax.numpy as jnp
import numpy as np
from jax import lax
from jax.experimental import pallas as pl
from jax.experimental.pallas import tpu as pltpu
from jax.sharding import PartitionSpec as P

VMEM_BYTES = 24 * 2**20
EPS_SCALE = 0.01
SENSOR_CENTRE = -3.0
SENSOR_WIDTH = 1.5
RATIO_FLOOR = 1e-06
ENERGY_EPS = 1e-06
GAUSS_NODES = [-0.906179845938664, -0.5384693101056831, 0.0, 0.5384693101056831, 0.906179845938664]
GAUSS_WEIGHTS = [
    0.2369268850561891,
    0.4786286704993665,
    0.5688888888888889,
    0.4786286704993665,
    0.2369268850561891,
]


def legendre_values(points):
    values = [np.ones(points.shape), np.array(points)]
    for order in range(1, 5):
        values.append(
            ((2 * order + 1) * points * values[order] - order * values[order - 1]) / (order + 1)
        )
    return values


def line_tables():
    line_nodes = np.array(GAUSS_NODES)
    quadrature_weights = np.array(GAUSS_WEIGHTS)
    barycentric = np.array(
        [
            1.0 / np.prod([line_nodes[j] - line_nodes[k] for k in range(5) if k != j])
            for j in range(5)
        ]
    )
    derivative = np.zeros((5, 5))
    for i in range(5):
        for j in range(5):
            if i != j:
                derivative[i, j] = barycentric[j] / barycentric[i] / (line_nodes[i] - line_nodes[j])
        derivative[i, i] = -np.sum(derivative[i])
    left_values = np.ones(5)
    right_values = np.ones(5)
    for j in range(5):
        for k in range(5):
            if k != j:
                left_values[j] *= (-1.0 - line_nodes[k]) / (line_nodes[j] - line_nodes[k])
                right_values[j] *= (1.0 - line_nodes[k]) / (line_nodes[j] - line_nodes[k])
    legendre = legendre_values(line_nodes)
    fourth_slope = 7.0 * legendre[3] + 3.0 * legendre[1]
    fifth_slope = 9.0 * legendre[4] + 5.0 * legendre[2] + legendre[0]
    left_corr = 0.5 * (fourth_slope - fifth_slope)
    right_corr = 0.5 * (fourth_slope + fifth_slope)
    modal = np.zeros((5, 5))
    for k in range(5):
        modal[k, :] = quadrature_weights * math.sqrt((2 * k + 1) / 2.0) * legendre[k]
    return (line_nodes, derivative, left_values, right_values, left_corr, right_corr, modal)


NODES, DERIV, LEFT, RIGHT, LIFT_LEFT, LIFT_RIGHT, MODAL = line_tables()
HALF_LEFT = 0.5 * LIFT_LEFT
HALF_RIGHT = 0.5 * LIFT_RIGHT


def fold(u):
    return (u[0] + u[4], u[1] + u[3], u[2], u[0] - u[4], u[1] - u[3])


def traces(parts):
    s0, s1, mid, d0, d1 = parts
    r = [float(x) for x in RIGHT]
    even = 0.5 * (r[0] + r[4]) * s0 + 0.5 * (r[1] + r[3]) * s1 + r[2] * mid
    odd = 0.5 * (r[0] - r[4]) * d0 + 0.5 * (r[1] - r[3]) * d1
    return even - odd, even + odd


def slope(parts, jump_left, jump_right):
    s0, s1, mid, d0, d1 = parts
    h = [float(x) for x in HALF_LEFT]
    diff = jump_left - jump_right
    both = jump_left + jump_right
    even, odd = [], []
    for i in range(3):
        even.append(
            float(0.5 * (DERIV[i, 0] - DERIV[i, 4])) * d0
            + float(0.5 * (DERIV[i, 1] - DERIV[i, 3])) * d1
            + 0.5 * (h[i] + h[4 - i]) * diff
        )
    for i in range(2):
        odd.append(
            float(0.5 * (DERIV[i, 0] + DERIV[i, 4])) * s0
            + float(0.5 * (DERIV[i, 1] + DERIV[i, 3])) * s1
            + float(DERIV[i, 2]) * mid
            + 0.5 * (h[i] - h[4 - i]) * both
        )
    return [even[0] + odd[0], even[1] + odd[1], even[2], even[1] - odd[1], even[0] - odd[0]]


def points(axis, q, j):
    if axis == 0:
        return [25 * i + 5 * q + j for i in range(5)]
    if axis == 1:
        return [25 * q + 5 * i + j for i in range(5)]
    return [25 * q + 5 * j + i for i in range(5)]


def modal_line(u):
    s0, s1, mid, d0, d1 = fold(u)
    out = []
    for k in range(5):
        m = [float(x) for x in MODAL[k]]
        out.append(m[0] * s0 + m[1] * s1 + m[2] * mid if k % 2 == 0 else m[0] * d0 + m[1] * d1)
    return out


def sensor(load, work):
    def first(q, carry):
        for j in range(5):
            pts = points(0, q, j)
            for i, value in zip(pts, modal_line([load(p) for p in pts])):
                work[i] = value
        return carry

    lax.fori_loop(0, 5, first, 0)

    def second(q, carry):
        total, high = carry
        plane = {}
        for c in range(5):
            for b, value in enumerate(modal_line([work[25 * q + 5 * b + c] for b in range(5)])):
                plane[b, c] = value
        low = jnp.zeros_like(total)
        edge = jnp.zeros_like(total)
        for b in range(5):
            line = modal_line([plane[b, c] for c in range(5)])
            squares = [x * x for x in line]
            if b < 4:
                low = low + ((squares[0] + squares[1]) + (squares[2] + squares[3]))
                edge = edge + squares[4]
            else:
                edge = edge + ((squares[0] + squares[1]) + (squares[2] + squares[3])) + squares[4]
        plane_total = low + edge
        return total + plane_total, high + jnp.where(q == 4, plane_total, edge)

    zero = jnp.zeros(work.shape[1:], jnp.float32)
    total, high = lax.fori_loop(0, 5, second, (zero, zero))
    level = jnp.log(jnp.maximum(high / (total + ENERGY_EPS), RATIO_FLOOR)) * (1.0 / math.log(10.0))
    ramp = jnp.clip((level - SENSOR_CENTRE) / SENSOR_WIDTH, -1.0, 1.0)
    return EPS_SCALE * 0.5 * (1.0 + jnp.sin(0.5 * math.pi * ramp))


def rolled(value, shift, axis):
    size = value.shape[axis]
    return pltpu.roll(value, shift % size, axis)


LOWER = [float((1.0 - x) / 2.0) for x in NODES]
UPPER = [float((1.0 + x) / 2.0) for x in NODES]


def along_lanes(line):
    lanes = line.shape[1]
    lane = lax.broadcasted_iota(jnp.int32, line.shape, 1)
    before = jnp.where(lane == 0, 0.0, rolled(line, 1, 1))
    after = jnp.where(lane == lanes - 1, 0.0, rolled(line, -1, 1))
    return jnp.maximum(line, before), jnp.maximum(line, after)


def interpolate(neighbours, nu):
    corner = {}
    for x in range(2):
        for y in range(2):
            line = jnp.maximum(
                jnp.maximum(neighbours[x][y], neighbours[x + 1][y]),
                jnp.maximum(neighbours[x][y + 1], neighbours[x + 1][y + 1]),
            )
            corner[x, y, 0], corner[x, y, 1] = along_lanes(line)
    lower, upper = LOWER, UPPER
    for a in range(5):
        face = {
            (y, z): lower[a] * corner[0, y, z] + upper[a] * corner[1, y, z]
            for y in range(2)
            for z in range(2)
        }
        for b in range(5):
            edge = [lower[b] * face[0, z] + upper[b] * face[1, z] for z in range(2)]
            for c in range(5):
                nu[25 * a + 5 * b + c] = lower[c] * edge[0] + upper[c] * edge[1]
    return corner


def row_masks(axis, chords, spans, lanes):
    row = lax.broadcasted_iota(jnp.int32, (chords * spans, lanes), 0)
    if axis == 0:
        return row < spans, row >= (chords - 1) * spans
    place = row % spans
    return place == 0, place == spans - 1


def outer_rows(axis, chords, spans, last):
    if axis == 0:
        return pl.ds((chords - 1) * spans if last else 0, spans)
    return pl.ds(spans - 1 if last else 0, chords, spans)


def store_pair(work, slot, left, right, down, up, index, rows_low, rows_high):
    work[2 * slot] = left
    work[2 * slot + 1] = right
    down[index] = work[2 * slot, rows_low]
    up[index] = work[2 * slot + 1, rows_high]


def local_kernel(sizes, count, chords, spans, *refs):
    state_hbm = refs[0]
    nu, result = refs[1:3]
    (
        state, acc, around, work, eps_out, faces_c, faces_s, gain, edge, beta, outside, alpha,
        t0, t1, t2, t3, f0, f1, f2, f3,
    ) = refs[3:23]
    ghosts, flux_ghosts = refs[23:27], refs[27:31]
    load_sem, store_sem, eps_send, eps_recv, send_sem, recv_sem = refs[31:]
    sends = ((t0, t1, t2, t3), (f0, f1, f2, f3))
    lands = (ghosts, flux_ghosts)
    rows, lanes = nu.shape[1:]
    chord_size, span_size = sizes
    me_c, me_s = lax.axis_index("chord"), lax.axis_index("span")
    mesh_id = pl.DeviceIdType.MESH

    def load(v):
        return pltpu.make_async_copy(state_hbm.at[v], state.at[v], load_sem.at[v])

    for v in range(count):
        load(v).start()

    def reachable(dx):
        if dx == 0:
            return None
        return me_c + 1 < chord_size if dx == 1 else me_c > 0

    def guarded(cond, run):
        if cond is None:
            run()
        else:
            pl.when(cond)(run)

    def partner(dx, dy):
        return (me_c + dx, lax.rem(me_s + dy + span_size, span_size))

    offsets = [(dx, dy) for dx in (0, -1, 1) for dy in (-1, 0, 1) if (dx, dy) != (0, 0)]
    barrier = pltpu.get_barrier_semaphore()
    for dx, dy in offsets:

        def greet(dx=dx, dy=dy):
            pl.semaphore_signal(barrier, inc=1, device_id=partner(dx, dy), device_id_type=mesh_id)

        guarded(reachable(dx), greet)

    def eps_copy(dx, dy):
        slot = 3 * (dx + 1) + dy + 1
        return pltpu.make_async_remote_copy(
            src_ref=eps_out, dst_ref=around.at[1 - dx, 1 - dy],
            send_sem=eps_send.at[slot], recv_sem=eps_recv.at[8 - slot],
            device_id=partner(dx, dy), device_id_type=mesh_id,
        )

    ways = ((1, 0), (-1, 0), (0, 1), (0, -1))

    def message(stage, k, v):
        dx, dy = ways[k]
        return pltpu.make_async_remote_copy(
            src_ref=sends[stage][k].at[v], dst_ref=lands[stage][k].at[v],
            send_sem=send_sem.at[stage, k, v], recv_sem=recv_sem.at[stage, k, v],
            device_id=partner(dx, dy), device_id_type=mesh_id,
        )

    def launch(stage, axis, v):
        for k in (2 * axis, 2 * axis + 1):
            guarded(reachable(ways[k][0]), lambda k=k: message(stage, k, v).start())

    masks = [row_masks(axis, chords, spans, lanes) for axis in range(2)]
    outer = [[outer_rows(axis, chords, spans, last) for last in (False, True)] for axis in range(2)]

    def send_traces(axis, v):
        up, down = sends[0][2 * axis], sends[0][2 * axis + 1]
        faces = (faces_c, faces_s)[axis]

        def body(q, carry):
            for j in range(5):
                left, right = traces(fold([state[v, p] for p in points(axis, q, j)]))
                faces[v, 5 * q + j] = jnp.where(masks[axis][0], left, right)
                store_pair(work, j, left, right, down, up, (v, 5 * q + j), *outer[axis])
            return carry

        lax.fori_loop(0, 5, body, 0)

    load(0).wait()
    send_traces(1, 0)
    sides = jnp.where(me_c > 0, 1, 0) + jnp.where(me_c + 1 < chord_size, 1, 0)
    pl.semaphore_wait(barrier, 2 + 3 * sides)
    launch(0, 1, 0)
    eps = sensor(lambda p: state[0, p], work)
    eps_out[...] = eps
    around[1, 1] = eps
    for dx, dy in offsets:
        guarded(reachable(dx), lambda dx=dx, dy=dy: eps_copy(dx, dy).start())

    send_traces(0, 0)
    launch(0, 0, 0)

    def later_traces(v, carry):
        load(v).wait()
        for axis in (1, 0):
            send_traces(axis, v)
            launch(0, axis, v)
        return carry

    lax.fori_loop(1, count, later_traces, 0)

    row = lax.broadcasted_iota(jnp.int32, (rows, lanes), 0)
    for dx, dy in offsets:
        guarded(reachable(-dx), lambda dx=dx, dy=dy: eps_copy(dx, dy).wait_recv())

    have_low = jnp.where(me_c > 0, spans, 0)
    have_high = jnp.where(me_c + 1 < chord_size, rows, rows - spans)
    low_s, high_s = masks[1]
    low_c, high_c = masks[0]
    column = []
    for x in range(3):
        mine, left, right = around[x, 1], around[x, 0], around[x, 2]
        column.append([
            jnp.where(low_s, rolled(left, 1 - spans, 0), rolled(mine, 1, 0)),
            mine,
            jnp.where(high_s, rolled(right, spans - 1, 0), rolled(mine, -1, 0)),
            jnp.where(low_s, rolled(left, 2 - spans, 0), rolled(right, spans - 2, 0)),
        ])
    closed_low = row < spans - have_low
    closed_high = row >= have_high
    neighbours = [[], [], [], []]
    for y in range(4):
        inner = column[1][y]
        below = jnp.where(low_c, rolled(column[0][y], spans, 0), rolled(inner, spans, 0))
        above = jnp.where(high_c, rolled(column[2][y], -spans, 0), rolled(inner, -spans, 0))
        beyond = jnp.where(
            low_c, rolled(column[0][y], 2 * spans, 0), rolled(column[2][y], -2 * spans, 0)
        )
        neighbours[0].append(jnp.where(closed_low, 0.0, below))
        neighbours[1].append(inner)
        neighbours[2].append(jnp.where(closed_high, 0.0, above))
        neighbours[3].append(beyond)
    corner = interpolate(neighbours, nu)
    near_weight = sum(float(LEFT[i] * HALF_LEFT[i] * (1.0 - NODES[i]) / 2.0) for i in range(5))
    far_weight = sum(float(LEFT[i] * HALF_LEFT[i] * (1.0 + NODES[i]) / 2.0) for i in range(5))
    for axis in range(2):
        low = masks[axis][0]
        sign = jnp.where(low, -1.0, 1.0)
        weight = {}
        for t in range(2):
            pair = []
            for o in (t, t + 1):
                if axis == 0:
                    pair += [jnp.where(low, neighbours[0][o], neighbours[2][o]), neighbours[3][o]]
                else:
                    pair += [jnp.where(low, neighbours[o][0], neighbours[o][2]), neighbours[o][3]]
            line = jnp.maximum(jnp.maximum(pair[0], pair[1]), jnp.maximum(pair[2], pair[3]))
            far = along_lanes(line)
            for z in range(2):
                if axis == 0:
                    near = jnp.where(low, corner[0, t, z], corner[1, t, z])
                else:
                    near = jnp.where(low, corner[t, 0, z], corner[t, 1, z])
                weight[t, z] = sign * (near_weight * near + far_weight * far[z])
        for m in range(5):
            ends = [LOWER[m] * weight[0, z] + UPPER[m] * weight[1, z] for z in range(2)]
            for c in range(5):
                beta[axis, 5 * m + c] = LOWER[c] * ends[0] + UPPER[c] * ends[1]

    for axis in (1, 0):

        def variable(v, carry):
            up, down = sends[1][2 * axis], sends[1][2 * axis + 1]
            low, high = masks[axis]
            step = spans if axis == 0 else 1

            def body(q, carry):
                for j in range(5):
                    pts = points(axis, q, j)
                    parts = fold([state[v, p] for p in pts])
                    left, right = traces(parts)
                    jump_left = jnp.where(low, 0.0, rolled(right, step, 0)) - left
                    jump_right = jnp.where(high, 0.0, rolled(left, -step, 0)) - right
                    if axis == 0:
                        jump_left = jnp.where(closed_low, 0.0, jump_left)
                        jump_right = jnp.where(closed_high, 0.0, jump_right)
                    gradient = slope(parts, jump_left, jump_right)
                    parts = fold([nu[p] * g for p, g in zip(pts, gradient)])
                    left, right = traces(parts)
                    store_pair(work, j, left, right, down, up, (v, 5 * q + j), *outer[axis])
                    before = jnp.where(low, 0.0, rolled(right, step, 0))
                    after = jnp.where(high, 0.0, rolled(left, -step, 0))
                    if axis == 0:
                        before = jnp.where(closed_low, -left, before)
                        after = jnp.where(closed_high, -right, after)
                    for p, value in zip(pts, slope(parts, before - left, after - right)):
                        if axis == 1:
                            acc[v, p] = value
                        else:
                            acc[v, p] += value
                return carry

            lax.fori_loop(0, 5, body, 0)
            launch(1, axis, v)
            return carry

        lax.fori_loop(0, count, variable, 0)

    lane = lax.broadcasted_iota(jnp.int32, (rows, lanes), 1)
    first, last = lane == 0, lane == lanes - 1

    def store(v):
        return pltpu.make_async_copy(acc.at[v], result.at[v], store_sem.at[v])

    for axis in range(2):
        low, high = masks[axis]

        def gains(q, carry):
            for j in range(5):
                f = 5 * q + j
                spread = []
                for i, p in enumerate(points(axis, q, j)):
                    lift = jnp.where(high, float(HALF_RIGHT[i]), 0.0)
                    spread.append(nu[p] * jnp.where(low, float(HALF_LEFT[i]), lift))
                parts = fold(spread)
                left, right = traces(parts)
                edge[axis, 2 * f] = left
                edge[axis, 2 * f + 1] = right
                for i, value in enumerate(slope(parts, -left, -right)):
                    gain[axis, 5 * f + i] = value
            return carry

        lax.fori_loop(0, 5, gains, 0)

    def normal(v, carry):
        def body(q, carry):
            for j in range(5):
                pts = points(2, q, j)
                parts = fold([state[v, p] for p in pts])
                left, right = traces(parts)
                jump_left = jnp.where(first, 0.0, rolled(right, 1, 1) - left)
                jump_right = jnp.where(last, 0.0, rolled(left, -1, 1) - right)
                gradient = slope(parts, jump_left, jump_right)
                parts = fold([nu[p] * g for p, g in zip(pts, gradient)])
                left, right = traces(parts)
                jump_left = jnp.where(first, -left, rolled(right, 1, 1)) - left
                jump_right = jnp.where(last, -right, rolled(left, -1, 1)) - right
                for p, value in zip(pts, slope(parts, jump_left, jump_right)):
                    acc[v, p] += value
            return carry

        lax.fori_loop(0, 5, body, 0)
        return carry

    lax.fori_loop(0, count, normal, 0)

    def arrived(axis, v):
        for k in (2 * axis, 2 * axis + 1):
            for stage in range(2):
                guarded(
                    reachable(-ways[k][0]),
                    lambda k=k, stage=stage: message(stage, k, v).wait_recv(),
                )

    for axis in (0, 1):

        def correct(v, carry):
            arrived(axis, v)
            up, down = ghosts[2 * axis], ghosts[2 * axis + 1]
            f_up, f_down = flux_ghosts[2 * axis], flux_ghosts[2 * axis + 1]
            faces = (faces_c, faces_s)[axis]
            low, high = masks[axis]
            rows_low, rows_high = outer[axis]
            step = spans if axis == 0 else 1
            opened = low | high
            if axis == 0:
                opened = opened & jnp.logical_not(closed_low | closed_high)

            def gather(q, carry):
                for j in range(5):
                    f = 5 * q + j
                    outside[f, rows_low] = up[v, f]
                    outside[f, rows_high] = down[v, f]
                    alpha[f, rows_low] = f_up[v, f]
                    alpha[f, rows_high] = f_down[v, f]
                return carry

            lax.fori_loop(0, 5, gather, 0)

            def body(q, carry):
                for j in range(5):
                    f = 5 * q + j
                    ghost = jnp.where(opened, outside[f], 0.0)
                    flux = jnp.where(opened, alpha[f] + beta[axis, f] * faces[v, f], 0.0)
                    before = jnp.where(low, flux, rolled(edge[axis, 2 * f + 1] * ghost, step, 0))
                    after = jnp.where(high, flux, rolled(edge[axis, 2 * f] * ghost, -step, 0))
                    h = [float(x) for x in HALF_LEFT]
                    diff, both = before - after, before + after
                    even = [0.5 * (h[i] + h[4 - i]) * diff for i in range(3)]
                    odd = [0.5 * (h[i] - h[4 - i]) * both for i in range(2)]
                    lifts = [
                        even[0] + odd[0], even[1] + odd[1], even[2],
                        even[1] - odd[1], even[0] - odd[0],
                    ]
                    for i, p in enumerate(points(axis, q, j)):
                        acc[v, p] += gain[axis, 5 * f + i] * ghost + lifts[i]
                return carry

            lax.fori_loop(0, 5, body, 0)
            if axis == 1:
                store(v).start()
            return carry

        lax.fori_loop(0, count, correct, 0)

    for v in range(count):
        store(v).wait()
    for dx, dy in offsets:
        guarded(reachable(dx), lambda dx=dx, dy=dy: eps_copy(dx, dy).wait_send())
    for stage in range(2):
        for k in range(4):
            for v in range(count):
                guarded(
                    reachable(ways[k][0]),
                    lambda stage=stage, k=k, v=v: message(stage, k, v).wait_send(),
                )


def shards(state):
    count, npts, chords, spans, lanes = state.shape
    rows = chords * spans
    flat = state.reshape(count, npts, rows, lanes)
    f32 = jnp.float32
    sizes = (lax.axis_size("chord"), lax.axis_size("span"))

    def message(n, k):
        return (n, 25, spans if k < 2 else chords, lanes)

    def full(*shape):
        return jax.ShapeDtypeStruct(shape, f32)

    vmem = pl.BlockSpec(memory_space=pltpu.VMEM)
    hbm = pl.BlockSpec(memory_space=pl.ANY)
    nu, residual = pl.pallas_call(
        functools.partial(local_kernel, sizes, count, chords, spans),
        in_specs=[pl.BlockSpec(memory_space=pltpu.HBM)],
        out_specs=[vmem, hbm],
        out_shape=[full(npts, rows, lanes), full(count, npts, rows, lanes)],
        scratch_shapes=[
            pltpu.VMEM(shape, f32)
            for shape in [
                (count, npts, rows, lanes),
                (count, npts, rows, lanes),
                (3, 3, rows, lanes),
                (npts, rows, lanes),
                (rows, lanes),
                (count, 25, rows, lanes),
                (count, 25, rows, lanes),
                (2, npts, rows, lanes),
                (2, 50, rows, lanes),
                (2, 25, rows, lanes),
                (25, rows, lanes),
                (25, rows, lanes),
            ]
            + [message(count, k) for k in range(4)] * 4
        ]
        + [
            pltpu.SemaphoreType.DMA((count,)),
            pltpu.SemaphoreType.DMA((count,)),
            pltpu.SemaphoreType.DMA((9,)),
            pltpu.SemaphoreType.DMA((9,)),
            pltpu.SemaphoreType.DMA((2, 4, count)),
            pltpu.SemaphoreType.DMA((2, 4, count)),
        ],
        compiler_params=pltpu.CompilerParams(
            collective_id=0, has_side_effects=True, vmem_limit_bytes=VMEM_BYTES
        ),
    )(flat)
    return residual.reshape(state.shape), nu.reshape(npts, chords, spans, lanes)


def solution(mesh):
    in_specs = (P(None, None, "chord", "span", None),)
    out_specs = (P(None, None, "chord", "span", None), P(None, "chord", "span", None))
    return jax.shard_map(shards, mesh=mesh, in_specs=in_specs, out_specs=out_specs, check_vma=False)
```

```python
import functools
import math

import jax
import jax.numpy as jnp
import numpy as np
from jax import lax
from jax.experimental import pallas as pl
from jax.experimental.pallas import tpu as pltpu
from jax.sharding import PartitionSpec as P

VMEM_BYTES = 24 * 2**20
EPS_SCALE = 0.01
SENSOR_CENTRE = -3.0
SENSOR_WIDTH = 1.5
RATIO_FLOOR = 1e-06
ENERGY_EPS = 1e-06
GAUSS_NODES = [-0.906179845938664, -0.5384693101056831, 0.0, 0.5384693101056831, 0.906179845938664]
GAUSS_WEIGHTS = [
    0.2369268850561891,
    0.4786286704993665,
    0.5688888888888889,
    0.4786286704993665,
    0.2369268850561891,
]


def legendre_values(points):
    values = [np.ones(points.shape), np.array(points)]
    for order in range(1, 5):
        values.append(
            ((2 * order + 1) * points * values[order] - order * values[order - 1]) / (order + 1)
        )
    return values


def line_tables():
    line_nodes = np.array(GAUSS_NODES)
    quadrature_weights = np.array(GAUSS_WEIGHTS)
    barycentric = np.array(
        [
            1.0 / np.prod([line_nodes[j] - line_nodes[k] for k in range(5) if k != j])
            for j in range(5)
        ]
    )
    derivative = np.zeros((5, 5))
    for i in range(5):
        for j in range(5):
            if i != j:
                derivative[i, j] = barycentric[j] / barycentric[i] / (line_nodes[i] - line_nodes[j])
        derivative[i, i] = -np.sum(derivative[i])
    left_values = np.ones(5)
    right_values = np.ones(5)
    for j in range(5):
        for k in range(5):
            if k != j:
                left_values[j] *= (-1.0 - line_nodes[k]) / (line_nodes[j] - line_nodes[k])
                right_values[j] *= (1.0 - line_nodes[k]) / (line_nodes[j] - line_nodes[k])
    legendre = legendre_values(line_nodes)
    fourth_slope = 7.0 * legendre[3] + 3.0 * legendre[1]
    fifth_slope = 9.0 * legendre[4] + 5.0 * legendre[2] + legendre[0]
    left_corr = 0.5 * (fourth_slope - fifth_slope)
    right_corr = 0.5 * (fourth_slope + fifth_slope)
    modal = np.zeros((5, 5))
    for k in range(5):
        modal[k, :] = quadrature_weights * math.sqrt((2 * k + 1) / 2.0) * legendre[k]
    return (line_nodes, derivative, left_values, right_values, left_corr, right_corr, modal)


NODES, DERIV, LEFT, RIGHT, LIFT_LEFT, LIFT_RIGHT, MODAL = line_tables()
HALF_LEFT = 0.5 * LIFT_LEFT
HALF_RIGHT = 0.5 * LIFT_RIGHT


def fold(u):
    return (u[0] + u[4], u[1] + u[3], u[2], u[0] - u[4], u[1] - u[3])


def traces(parts):
    s0, s1, mid, d0, d1 = parts
    r = [float(x) for x in RIGHT]
    even = 0.5 * (r[0] + r[4]) * s0 + 0.5 * (r[1] + r[3]) * s1 + r[2] * mid
    odd = 0.5 * (r[0] - r[4]) * d0 + 0.5 * (r[1] - r[3]) * d1
    return even - odd, even + odd


def slope(parts, jump_left, jump_right):
    s0, s1, mid, d0, d1 = parts
    h = [float(x) for x in HALF_LEFT]
    diff = jump_left - jump_right
    both = jump_left + jump_right
    even, odd = [], []
    for i in range(3):
        even.append(
            float(0.5 * (DERIV[i, 0] - DERIV[i, 4])) * d0
            + float(0.5 * (DERIV[i, 1] - DERIV[i, 3])) * d1
            + 0.5 * (h[i] + h[4 - i]) * diff
        )
    for i in range(2):
        odd.append(
            float(0.5 * (DERIV[i, 0] + DERIV[i, 4])) * s0
            + float(0.5 * (DERIV[i, 1] + DERIV[i, 3])) * s1
            + float(DERIV[i, 2]) * mid
            + 0.5 * (h[i] - h[4 - i]) * both
        )
    return [even[0] + odd[0], even[1] + odd[1], even[2], even[1] - odd[1], even[0] - odd[0]]


def points(axis, q, j):
    if axis == 0:
        return [25 * i + 5 * q + j for i in range(5)]
    if axis == 1:
        return [25 * q + 5 * i + j for i in range(5)]
    return [25 * q + 5 * j + i for i in range(5)]


def modal_line(u):
    s0, s1, mid, d0, d1 = fold(u)
    out = []
    for k in range(5):
        m = [float(x) for x in MODAL[k]]
        out.append(m[0] * s0 + m[1] * s1 + m[2] * mid if k % 2 == 0 else m[0] * d0 + m[1] * d1)
    return out


def sensor(load, work):
    def first(q, carry):
        for j in range(5):
            pts = points(0, q, j)
            for i, value in zip(pts, modal_line([load(p) for p in pts])):
                work[i] = value
        return carry

    lax.fori_loop(0, 5, first, 0)

    def second(q, carry):
        total, high = carry
        plane = {}
        for c in range(5):
            for b, value in enumerate(modal_line([work[25 * q + 5 * b + c] for b in range(5)])):
                plane[b, c] = value
        low = jnp.zeros_like(total)
        edge = jnp.zeros_like(total)
        for b in range(5):
            line = modal_line([plane[b, c] for c in range(5)])
            squares = [x * x for x in line]
            if b < 4:
                low = low + ((squares[0] + squares[1]) + (squares[2] + squares[3]))
                edge = edge + squares[4]
            else:
                edge = edge + ((squares[0] + squares[1]) + (squares[2] + squares[3])) + squares[4]
        plane_total = low + edge
        return total + plane_total, high + jnp.where(q == 4, plane_total, edge)

    zero = jnp.zeros(work.shape[1:], jnp.float32)
    total, high = lax.fori_loop(0, 5, second, (zero, zero))
    level = jnp.log(jnp.maximum(high / (total + ENERGY_EPS), RATIO_FLOOR)) * (1.0 / math.log(10.0))
    ramp = jnp.clip((level - SENSOR_CENTRE) / SENSOR_WIDTH, -1.0, 1.0)
    return EPS_SCALE * 0.5 * (1.0 + jnp.sin(0.5 * math.pi * ramp))


def rolled(value, shift, axis):
    size = value.shape[axis]
    return pltpu.roll(value, shift % size, axis)


LOWER = [float((1.0 - x) / 2.0) for x in NODES]
UPPER = [float((1.0 + x) / 2.0) for x in NODES]


def along_lanes(line):
    lanes = line.shape[1]
    lane = lax.broadcasted_iota(jnp.int32, line.shape, 1)
    before = jnp.where(lane == 0, 0.0, rolled(line, 1, 1))
    after = jnp.where(lane == lanes - 1, 0.0, rolled(line, -1, 1))
    return jnp.maximum(line, before), jnp.maximum(line, after)


def interpolate(neighbours, nu):
    corner = {}
    for x in range(2):
        for y in range(2):
            line = jnp.maximum(
                jnp.maximum(neighbours[x][y], neighbours[x + 1][y]),
                jnp.maximum(neighbours[x][y + 1], neighbours[x + 1][y + 1]),
            )
            corner[x, y, 0], corner[x, y, 1] = along_lanes(line)
    lower, upper = LOWER, UPPER
    for a in range(5):
        face = {
            (y, z): lower[a] * corner[0, y, z] + upper[a] * corner[1, y, z]
            for y in range(2)
            for z in range(2)
        }
        for b in range(5):
            edge = [lower[b] * face[0, z] + upper[b] * face[1, z] for z in range(2)]
            for c in range(5):
                nu[25 * a + 5 * b + c] = lower[c] * edge[0] + upper[c] * edge[1]
    return corner


def row_masks(axis, chords, spans, lanes):
    row = lax.broadcasted_iota(jnp.int32, (chords * spans, lanes), 0)
    if axis == 0:
        return row < spans, row >= (chords - 1) * spans
    place = row % spans
    return place == 0, place == spans - 1


def outer_rows(axis, chords, spans, last):
    if axis == 0:
        return pl.ds((chords - 1) * spans if last else 0, spans)
    return pl.ds(spans - 1 if last else 0, chords, spans)


def store_pair(work, slot, left, right, down, up, index, rows_low, rows_high):
    work[2 * slot] = left
    work[2 * slot + 1] = right
    down[index] = work[2 * slot, rows_low]
    up[index] = work[2 * slot + 1, rows_high]


def local_kernel(sizes, count, chords, spans, *refs):
    state = refs[0]
    nu, acc = refs[1:3]
    (
        around, work, eps_out, faces_c, faces_s, gain, edge, beta, outside, alpha,
        t0, t1, t2, t3, f0, f1, f2, f3,
    ) = refs[3:21]
    ghosts, flux_ghosts = refs[21:25], refs[25:29]
    eps_send, eps_recv, send_sem, recv_sem = refs[29:]
    sends = ((t0, t1, t2, t3), (f0, f1, f2, f3))
    lands = (ghosts, flux_ghosts)
    rows, lanes = nu.shape[1:]
    chord_size, span_size = sizes
    me_c, me_s = lax.axis_index("chord"), lax.axis_index("span")
    mesh_id = pl.DeviceIdType.MESH

    def reachable(dx):
        if dx == 0:
            return None
        return me_c + 1 < chord_size if dx == 1 else me_c > 0

    def guarded(cond, run):
        if cond is None:
            run()
        else:
            pl.when(cond)(run)

    def partner(dx, dy):
        return (me_c + dx, lax.rem(me_s + dy + span_size, span_size))

    offsets = [(dx, dy) for dx in (0, -1, 1) for dy in (-1, 0, 1) if (dx, dy) != (0, 0)]
    barrier = pltpu.get_barrier_semaphore()
    for dx, dy in offsets:

        def greet(dx=dx, dy=dy):
            pl.semaphore_signal(barrier, inc=1, device_id=partner(dx, dy), device_id_type=mesh_id)

        guarded(reachable(dx), greet)

    def eps_copy(dx, dy):
        slot = 3 * (dx + 1) + dy + 1
        return pltpu.make_async_remote_copy(
            src_ref=eps_out, dst_ref=around.at[1 - dx, 1 - dy],
            send_sem=eps_send.at[slot], recv_sem=eps_recv.at[8 - slot],
            device_id=partner(dx, dy), device_id_type=mesh_id,
        )

    ways = ((1, 0), (-1, 0), (0, 1), (0, -1))

    def message(stage, k, v):
        dx, dy = ways[k]
        return pltpu.make_async_remote_copy(
            src_ref=sends[stage][k].at[v], dst_ref=lands[stage][k].at[v],
            send_sem=send_sem.at[stage, k, v], recv_sem=recv_sem.at[stage, k, v],
            device_id=partner(dx, dy), device_id_type=mesh_id,
        )

    def launch(stage, axis, v):
        for k in (2 * axis, 2 * axis + 1):
            guarded(reachable(ways[k][0]), lambda k=k: message(stage, k, v).start())

    masks = [row_masks(axis, chords, spans, lanes) for axis in range(2)]
    outer = [[outer_rows(axis, chords, spans, last) for last in (False, True)] for axis in range(2)]

    def send_traces(axis, v):
        up, down = sends[0][2 * axis], sends[0][2 * axis + 1]
        faces = (faces_c, faces_s)[axis]

        def body(q, carry):
            for j in range(5):
                left, right = traces(fold([state[v, p] for p in points(axis, q, j)]))
                faces[v, 5 * q + j] = jnp.where(masks[axis][0], left, right)
                store_pair(work, j, left, right, down, up, (v, 5 * q + j), *outer[axis])
            return carry

        lax.fori_loop(0, 5, body, 0)

    send_traces(1, 0)
    sides = jnp.where(me_c > 0, 1, 0) + jnp.where(me_c + 1 < chord_size, 1, 0)
    pl.semaphore_wait(barrier, 2 + 3 * sides)
    launch(0, 1, 0)
    eps = sensor(lambda p: state[0, p], work)
    eps_out[...] = eps
    around[1, 1] = eps
    for dx, dy in offsets:
        guarded(reachable(dx), lambda dx=dx, dy=dy: eps_copy(dx, dy).start())

    send_traces(0, 0)
    launch(0, 0, 0)

    def later_traces(v, carry):
        for axis in (1, 0):
            send_traces(axis, v)
            launch(0, axis, v)
        return carry

    lax.fori_loop(1, count, later_traces, 0)

    row = lax.broadcasted_iota(jnp.int32, (rows, lanes), 0)
    for dx, dy in offsets:
        guarded(reachable(-dx), lambda dx=dx, dy=dy: eps_copy(dx, dy).wait_recv())

    have_low = jnp.where(me_c > 0, spans, 0)
    have_high = jnp.where(me_c + 1 < chord_size, rows, rows - spans)
    low_s, high_s = masks[1]
    low_c, high_c = masks[0]
    column = []
    for x in range(3):
        mine, left, right = around[x, 1], around[x, 0], around[x, 2]
        column.append([
            jnp.where(low_s, rolled(left, 1 - spans, 0), rolled(mine, 1, 0)),
            mine,
            jnp.where(high_s, rolled(right, spans - 1, 0), rolled(mine, -1, 0)),
            jnp.where(low_s, rolled(left, 2 - spans, 0), rolled(right, spans - 2, 0)),
        ])
    closed_low = row < spans - have_low
    closed_high = row >= have_high
    neighbours = [[], [], [], []]
    for y in range(4):
        inner = column[1][y]
        below = jnp.where(low_c, rolled(column[0][y], spans, 0), rolled(inner, spans, 0))
        above = jnp.where(high_c, rolled(column[2][y], -spans, 0), rolled(inner, -spans, 0))
        beyond = jnp.where(
            low_c, rolled(column[0][y], 2 * spans, 0), rolled(column[2][y], -2 * spans, 0)
        )
        neighbours[0].append(jnp.where(closed_low, 0.0, below))
        neighbours[1].append(inner)
        neighbours[2].append(jnp.where(closed_high, 0.0, above))
        neighbours[3].append(beyond)
    corner = interpolate(neighbours, nu)
    near_weight = sum(float(LEFT[i] * HALF_LEFT[i] * (1.0 - NODES[i]) / 2.0) for i in range(5))
    far_weight = sum(float(LEFT[i] * HALF_LEFT[i] * (1.0 + NODES[i]) / 2.0) for i in range(5))
    for axis in range(2):
        low = masks[axis][0]
        sign = jnp.where(low, -1.0, 1.0)
        weight = {}
        for t in range(2):
            pair = []
            for o in (t, t + 1):
                if axis == 0:
                    pair += [jnp.where(low, neighbours[0][o], neighbours[2][o]), neighbours[3][o]]
                else:
                    pair += [jnp.where(low, neighbours[o][0], neighbours[o][2]), neighbours[o][3]]
            line = jnp.maximum(jnp.maximum(pair[0], pair[1]), jnp.maximum(pair[2], pair[3]))
            far = along_lanes(line)
            for z in range(2):
                if axis == 0:
                    near = jnp.where(low, corner[0, t, z], corner[1, t, z])
                else:
                    near = jnp.where(low, corner[t, 0, z], corner[t, 1, z])
                weight[t, z] = sign * (near_weight * near + far_weight * far[z])
        for m in range(5):
            ends = [LOWER[m] * weight[0, z] + UPPER[m] * weight[1, z] for z in range(2)]
            for c in range(5):
                beta[axis, 5 * m + c] = LOWER[c] * ends[0] + UPPER[c] * ends[1]

    for axis in (1, 0):

        def variable(v, carry):
            up, down = sends[1][2 * axis], sends[1][2 * axis + 1]
            low, high = masks[axis]
            step = spans if axis == 0 else 1

            def body(q, carry):
                for j in range(5):
                    pts = points(axis, q, j)
                    parts = fold([state[v, p] for p in pts])
                    left, right = traces(parts)
                    jump_left = jnp.where(low, 0.0, rolled(right, step, 0)) - left
                    jump_right = jnp.where(high, 0.0, rolled(left, -step, 0)) - right
                    if axis == 0:
                        jump_left = jnp.where(closed_low, 0.0, jump_left)
                        jump_right = jnp.where(closed_high, 0.0, jump_right)
                    gradient = slope(parts, jump_left, jump_right)
                    parts = fold([nu[p] * g for p, g in zip(pts, gradient)])
                    left, right = traces(parts)
                    store_pair(work, j, left, right, down, up, (v, 5 * q + j), *outer[axis])
                    before = jnp.where(low, 0.0, rolled(right, step, 0))
                    after = jnp.where(high, 0.0, rolled(left, -step, 0))
                    if axis == 0:
                        before = jnp.where(closed_low, -left, before)
                        after = jnp.where(closed_high, -right, after)
                    for p, value in zip(pts, slope(parts, before - left, after - right)):
                        if axis == 1:
                            acc[v, p] = value
                        else:
                            acc[v, p] += value
                return carry

            lax.fori_loop(0, 5, body, 0)
            launch(1, axis, v)
            return carry

        lax.fori_loop(0, count, variable, 0)

    lane = lax.broadcasted_iota(jnp.int32, (rows, lanes), 1)
    first, last = lane == 0, lane == lanes - 1

    for axis in range(2):
        low, high = masks[axis]

        def gains(q, carry):
            for j in range(5):
                f = 5 * q + j
                spread = []
                for i, p in enumerate(points(axis, q, j)):
                    lift = jnp.where(high, float(HALF_RIGHT[i]), 0.0)
                    spread.append(nu[p] * jnp.where(low, float(HALF_LEFT[i]), lift))
                parts = fold(spread)
                left, right = traces(parts)
                edge[axis, 2 * f] = left
                edge[axis, 2 * f + 1] = right
                for i, value in enumerate(slope(parts, -left, -right)):
                    gain[axis, 5 * f + i] = value
            return carry

        lax.fori_loop(0, 5, gains, 0)

    def normal(v, carry):
        def body(q, carry):
            for j in range(5):
                pts = points(2, q, j)
                parts = fold([state[v, p] for p in pts])
                left, right = traces(parts)
                jump_left = jnp.where(first, 0.0, rolled(right, 1, 1) - left)
                jump_right = jnp.where(last, 0.0, rolled(left, -1, 1) - right)
                gradient = slope(parts, jump_left, jump_right)
                parts = fold([nu[p] * g for p, g in zip(pts, gradient)])
                left, right = traces(parts)
                jump_left = jnp.where(first, -left, rolled(right, 1, 1)) - left
                jump_right = jnp.where(last, -right, rolled(left, -1, 1)) - right
                for p, value in zip(pts, slope(parts, jump_left, jump_right)):
                    acc[v, p] += value
            return carry

        lax.fori_loop(0, 5, body, 0)
        return carry

    lax.fori_loop(0, count, normal, 0)

    def arrived(axis, v):
        for k in (2 * axis, 2 * axis + 1):
            for stage in range(2):
                guarded(
                    reachable(-ways[k][0]),
                    lambda k=k, stage=stage: message(stage, k, v).wait_recv(),
                )

    for axis in (0, 1):

        def correct(v, carry):
            arrived(axis, v)
            up, down = ghosts[2 * axis], ghosts[2 * axis + 1]
            f_up, f_down = flux_ghosts[2 * axis], flux_ghosts[2 * axis + 1]
            faces = (faces_c, faces_s)[axis]
            low, high = masks[axis]
            rows_low, rows_high = outer[axis]
            step = spans if axis == 0 else 1
            opened = low | high
            if axis == 0:
                opened = opened & jnp.logical_not(closed_low | closed_high)

            def gather(q, carry):
                for j in range(5):
                    f = 5 * q + j
                    outside[f, rows_low] = up[v, f]
                    outside[f, rows_high] = down[v, f]
                    alpha[f, rows_low] = f_up[v, f]
                    alpha[f, rows_high] = f_down[v, f]
                return carry

            lax.fori_loop(0, 5, gather, 0)

            def body(q, carry):
                for j in range(5):
                    f = 5 * q + j
                    ghost = jnp.where(opened, outside[f], 0.0)
                    flux = jnp.where(opened, alpha[f] + beta[axis, f] * faces[v, f], 0.0)
                    before = jnp.where(low, flux, rolled(edge[axis, 2 * f + 1] * ghost, step, 0))
                    after = jnp.where(high, flux, rolled(edge[axis, 2 * f] * ghost, -step, 0))
                    h = [float(x) for x in HALF_LEFT]
                    diff, both = before - after, before + after
                    even = [0.5 * (h[i] + h[4 - i]) * diff for i in range(3)]
                    odd = [0.5 * (h[i] - h[4 - i]) * both for i in range(2)]
                    lifts = [
                        even[0] + odd[0], even[1] + odd[1], even[2],
                        even[1] - odd[1], even[0] - odd[0],
                    ]
                    for i, p in enumerate(points(axis, q, j)):
                        acc[v, p] += gain[axis, 5 * f + i] * ghost + lifts[i]
                return carry

            lax.fori_loop(0, 5, body, 0)
            return carry

        lax.fori_loop(0, count, correct, 0)

    for dx, dy in offsets:
        guarded(reachable(dx), lambda dx=dx, dy=dy: eps_copy(dx, dy).wait_send())
    for stage in range(2):
        for k in range(4):
            for v in range(count):
                guarded(
                    reachable(ways[k][0]),
                    lambda stage=stage, k=k, v=v: message(stage, k, v).wait_send(),
                )


def shards(state):
    count, npts, chords, spans, lanes = state.shape
    rows = chords * spans
    flat = state.reshape(count, npts, rows, lanes)
    f32 = jnp.float32
    sizes = (lax.axis_size("chord"), lax.axis_size("span"))

    def message(n, k):
        return (n, 25, spans if k < 2 else chords, lanes)

    def full(*shape):
        return jax.ShapeDtypeStruct(shape, f32)

    vmem = pl.BlockSpec(memory_space=pltpu.VMEM)
    nu, residual = pl.pallas_call(
        functools.partial(local_kernel, sizes, count, chords, spans),
        in_specs=[vmem],
        out_specs=[vmem, vmem],
        out_shape=[full(npts, rows, lanes), full(count, npts, rows, lanes)],
        scratch_shapes=[
            pltpu.VMEM(shape, f32)
            for shape in [
                (3, 3, rows, lanes),
                (npts, rows, lanes),
                (rows, lanes),
                (count, 25, rows, lanes),
                (count, 25, rows, lanes),
                (2, npts, rows, lanes),
                (2, 50, rows, lanes),
                (2, 25, rows, lanes),
                (25, rows, lanes),
                (25, rows, lanes),
            ]
            + [message(count, k) for k in range(4)] * 4
        ]
        + [
            pltpu.SemaphoreType.DMA((9,)),
            pltpu.SemaphoreType.DMA((9,)),
            pltpu.SemaphoreType.DMA((2, 4, count)),
            pltpu.SemaphoreType.DMA((2, 4, count)),
        ],
        compiler_params=pltpu.CompilerParams(
            collective_id=0, has_side_effects=True, vmem_limit_bytes=VMEM_BYTES
        ),
    )(flat)
    return residual.reshape(state.shape), nu.reshape(npts, chords, spans, lanes)


def solution(mesh):
    in_specs = (P(None, None, "chord", "span", None),)
    out_specs = (P(None, None, "chord", "span", None), P(None, "chord", "span", None))
    return jax.shard_map(shards, mesh=mesh, in_specs=in_specs, out_specs=out_specs, check_vma=False)
```

```python
import functools
import math

import jax
import jax.numpy as jnp
import numpy as np
from jax import lax
from jax.experimental import pallas as pl
from jax.experimental.pallas import tpu as pltpu
from jax.sharding import PartitionSpec as P

VMEM_BYTES = 52_500_000
EPS_SCALE = 0.01
SENSOR_CENTRE = -3.0
SENSOR_WIDTH = 1.5
RATIO_FLOOR = 1e-06
ENERGY_EPS = 1e-06
GAUSS_NODES = [-0.906179845938664, -0.5384693101056831, 0.0, 0.5384693101056831, 0.906179845938664]
GAUSS_WEIGHTS = [
    0.2369268850561891,
    0.4786286704993665,
    0.5688888888888889,
    0.4786286704993665,
    0.2369268850561891,
]


def legendre_values(points):
    values = [np.ones(points.shape), np.array(points)]
    for order in range(1, 5):
        values.append(
            ((2 * order + 1) * points * values[order] - order * values[order - 1]) / (order + 1)
        )
    return values


def line_tables():
    line_nodes = np.array(GAUSS_NODES)
    quadrature_weights = np.array(GAUSS_WEIGHTS)
    barycentric = np.array(
        [
            1.0 / np.prod([line_nodes[j] - line_nodes[k] for k in range(5) if k != j])
            for j in range(5)
        ]
    )
    derivative = np.zeros((5, 5))
    for i in range(5):
        for j in range(5):
            if i != j:
                derivative[i, j] = barycentric[j] / barycentric[i] / (line_nodes[i] - line_nodes[j])
        derivative[i, i] = -np.sum(derivative[i])
    left_values = np.ones(5)
    right_values = np.ones(5)
    for j in range(5):
        for k in range(5):
            if k != j:
                left_values[j] *= (-1.0 - line_nodes[k]) / (line_nodes[j] - line_nodes[k])
                right_values[j] *= (1.0 - line_nodes[k]) / (line_nodes[j] - line_nodes[k])
    legendre = legendre_values(line_nodes)
    fourth_slope = 7.0 * legendre[3] + 3.0 * legendre[1]
    fifth_slope = 9.0 * legendre[4] + 5.0 * legendre[2] + legendre[0]
    left_corr = 0.5 * (fourth_slope - fifth_slope)
    right_corr = 0.5 * (fourth_slope + fifth_slope)
    modal = np.zeros((5, 5))
    for k in range(5):
        modal[k, :] = quadrature_weights * math.sqrt((2 * k + 1) / 2.0) * legendre[k]
    return (line_nodes, derivative, left_values, right_values, left_corr, right_corr, modal)


NODES, DERIV, LEFT, RIGHT, LIFT_LEFT, LIFT_RIGHT, MODAL = line_tables()
HALF_LEFT = 0.5 * LIFT_LEFT
HALF_RIGHT = 0.5 * LIFT_RIGHT


def fold(u):
    return (u[0] + u[4], u[1] + u[3], u[2], u[0] - u[4], u[1] - u[3])


def traces(parts):
    s0, s1, mid, d0, d1 = parts
    r = [float(x) for x in RIGHT]
    even = 0.5 * (r[0] + r[4]) * s0 + 0.5 * (r[1] + r[3]) * s1 + r[2] * mid
    odd = 0.5 * (r[0] - r[4]) * d0 + 0.5 * (r[1] - r[3]) * d1
    return even - odd, even + odd


def slope(parts, before, after):
    s0, s1, mid, d0, d1 = parts
    h = [float(x) for x in HALF_LEFT]
    r = [float(x) for x in RIGHT]
    if before is not None:
        diff, both = before - after, before + after
    even, odd = [], []
    for i in range(3):
        lift = 0.5 * (h[i] + h[4 - i])
        value = (
            float(0.5 * (DERIV[i, 0] - DERIV[i, 4]) + lift * (r[0] - r[4])) * d0
            + float(0.5 * (DERIV[i, 1] - DERIV[i, 3]) + lift * (r[1] - r[3])) * d1
        )
        even.append(value if before is None else value + lift * diff)
    for i in range(2):
        lift = 0.5 * (h[i] - h[4 - i])
        value = (
            float(0.5 * (DERIV[i, 0] + DERIV[i, 4]) - lift * (r[0] + r[4])) * s0
            + float(0.5 * (DERIV[i, 1] + DERIV[i, 3]) - lift * (r[1] + r[3])) * s1
            + float(DERIV[i, 2] - 2.0 * lift * r[2]) * mid
        )
        odd.append(value if before is None else value + lift * both)
    return [even[0] + odd[0], even[1] + odd[1], even[2], even[1] - odd[1], even[0] - odd[0]]


def points(axis, q, j):
    if axis == 0:
        return [25 * i + 5 * q + j for i in range(5)]
    if axis == 1:
        return [25 * q + 5 * i + j for i in range(5)]
    return [25 * q + 5 * j + i for i in range(5)]


def modal_line(u):
    s0, s1, mid, d0, d1 = fold(u)
    out = []
    for k in range(5):
        m = [float(x) for x in MODAL[k]]
        out.append(m[0] * s0 + m[1] * s1 + m[2] * mid if k % 2 == 0 else m[0] * d0 + m[1] * d1)
    return out


def sensor(load, work):
    def first(q, carry):
        for j in range(5):
            pts = points(0, q, j)
            for i, value in zip(pts, modal_line([load(p) for p in pts])):
                work[i] = value
        return carry

    lax.fori_loop(0, 5, first, 0)

    def second(q, carry):
        total, high = carry
        plane = {}
        for c in range(5):
            for b, value in enumerate(modal_line([work[25 * q + 5 * b + c] for b in range(5)])):
                plane[b, c] = value
        low = jnp.zeros_like(total)
        edge = jnp.zeros_like(total)
        for b in range(5):
            line = modal_line([plane[b, c] for c in range(5)])
            squares = [x * x for x in line]
            if b < 4:
                low = low + ((squares[0] + squares[1]) + (squares[2] + squares[3]))
                edge = edge + squares[4]
            else:
                edge = edge + ((squares[0] + squares[1]) + (squares[2] + squares[3])) + squares[4]
        plane_total = low + edge
        return total + plane_total, high + jnp.where(q == 4, plane_total, edge)

    zero = jnp.zeros(work.shape[1:], jnp.float32)
    total, high = lax.fori_loop(0, 5, second, (zero, zero))
    level = jnp.log(jnp.maximum(high / (total + ENERGY_EPS), RATIO_FLOOR)) * (1.0 / math.log(10.0))
    ramp = jnp.clip((level - SENSOR_CENTRE) / SENSOR_WIDTH, -1.0, 1.0)
    return EPS_SCALE * 0.5 * (1.0 + jnp.sin(0.5 * math.pi * ramp))


def rolled(value, shift, axis):
    size = value.shape[axis]
    return pltpu.roll(value, shift % size, axis)


LOWER = [float((1.0 - x) / 2.0) for x in NODES]
UPPER = [float((1.0 + x) / 2.0) for x in NODES]


def along_lanes(line):
    lanes = line.shape[1]
    lane = lax.broadcasted_iota(jnp.int32, line.shape, 1)
    before = jnp.where(lane == 0, 0.0, rolled(line, 1, 1))
    after = jnp.where(lane == lanes - 1, 0.0, rolled(line, -1, 1))
    return jnp.maximum(line, before), jnp.maximum(line, after)


def interpolate(neighbours, nu):
    corner = {}
    for x in range(2):
        for y in range(2):
            line = jnp.maximum(
                jnp.maximum(neighbours[x][y], neighbours[x + 1][y]),
                jnp.maximum(neighbours[x][y + 1], neighbours[x + 1][y + 1]),
            )
            corner[x, y, 0], corner[x, y, 1] = along_lanes(line)
    lower, upper = LOWER, UPPER
    for a in range(5):
        face = {
            (y, z): lower[a] * corner[0, y, z] + upper[a] * corner[1, y, z]
            for y in range(2)
            for z in range(2)
        }
        for b in range(5):
            edge = [lower[b] * face[0, z] + upper[b] * face[1, z] for z in range(2)]
            for c in range(5):
                nu[25 * a + 5 * b + c] = lower[c] * edge[0] + upper[c] * edge[1]
    return corner


def row_masks(axis, chords, spans, lanes):
    row = lax.broadcasted_iota(jnp.int32, (chords * spans, lanes), 0)
    if axis == 0:
        return row < spans, row >= (chords - 1) * spans
    place = row % spans
    return place == 0, place == spans - 1


def outer_rows(axis, chords, spans, last):
    if axis == 0:
        return pl.ds((chords - 1) * spans if last else 0, spans)
    return pl.ds(spans - 1 if last else 0, chords, spans)


def store_pair(work, slot, left, right, down, up, index, rows_low, rows_high):
    work[2 * slot] = left
    work[2 * slot + 1] = right
    down[index] = work[2 * slot, rows_low]
    up[index] = work[2 * slot + 1, rows_high]


def local_kernel(sizes, count, chords, spans, *refs):
    state_hbm = refs[0]
    nu, acc = refs[1:3]
    (
        state, grad, around, work, eps_out, faces_c, faces_s, gain, edge, beta, outside, alpha,
        t0, t1, t2, t3, f0, f1, f2, f3,
    ) = refs[3:23]
    ghosts, flux_ghosts = refs[23:27], refs[27:31]
    load_sem, eps_send, eps_recv, send_sem, recv_sem = refs[31:]
    sends = ((t0, t1, t2, t3), (f0, f1, f2, f3))
    lands = (ghosts, flux_ghosts)
    rows, lanes = nu.shape[1:]
    chord_size, span_size = sizes
    me_c, me_s = lax.axis_index("chord"), lax.axis_index("span")
    mesh_id = pl.DeviceIdType.MESH

    def load(v):
        return pltpu.make_async_copy(state_hbm.at[v], state.at[v], load_sem.at[v])

    for v in range(count):
        load(v).start()

    def reachable(dx):
        if dx == 0:
            return None
        return me_c + 1 < chord_size if dx == 1 else me_c > 0

    def guarded(cond, run):
        if cond is None:
            run()
        else:
            pl.when(cond)(run)

    def partner(dx, dy):
        return (me_c + dx, lax.rem(me_s + dy + span_size, span_size))

    offsets = [(dx, dy) for dx in (0, -1, 1) for dy in (-1, 0, 1) if (dx, dy) != (0, 0)]
    barrier = pltpu.get_barrier_semaphore()
    for dx, dy in offsets:

        def greet(dx=dx, dy=dy):
            pl.semaphore_signal(barrier, inc=1, device_id=partner(dx, dy), device_id_type=mesh_id)

        guarded(reachable(dx), greet)

    def eps_copy(dx, dy):
        slot = 3 * (dx + 1) + dy + 1
        return pltpu.make_async_remote_copy(
            src_ref=eps_out, dst_ref=around.at[1 - dx, 1 - dy],
            send_sem=eps_send.at[slot], recv_sem=eps_recv.at[8 - slot],
            device_id=partner(dx, dy), device_id_type=mesh_id,
        )

    ways = ((1, 0), (-1, 0), (0, 1), (0, -1))

    def message(stage, k, v):
        dx, dy = ways[k]
        return pltpu.make_async_remote_copy(
            src_ref=sends[stage][k].at[v], dst_ref=lands[stage][k].at[v],
            send_sem=send_sem.at[stage, k, v], recv_sem=recv_sem.at[stage, k, v],
            device_id=partner(dx, dy), device_id_type=mesh_id,
        )

    def launch(stage, axis, v):
        for k in (2 * axis, 2 * axis + 1):
            guarded(reachable(ways[k][0]), lambda k=k: message(stage, k, v).start())

    masks = [row_masks(axis, chords, spans, lanes) for axis in range(2)]
    outer = [[outer_rows(axis, chords, spans, last) for last in (False, True)] for axis in range(2)]

    def send_traces(axis, v):
        up, down = sends[0][2 * axis], sends[0][2 * axis + 1]
        faces = (faces_c, faces_s)[axis]

        def body(q, carry):
            for j in range(5):
                left, right = traces(fold([state[v, p] for p in points(axis, q, j)]))
                faces[v, 5 * q + j] = jnp.where(masks[axis][0], left, right)
                store_pair(work, j, left, right, down, up, (v, 5 * q + j), *outer[axis])
            return carry

        lax.fori_loop(0, 5, body, 0)

    load(0).wait()
    send_traces(1, 0)
    sides = jnp.where(me_c > 0, 1, 0) + jnp.where(me_c + 1 < chord_size, 1, 0)
    pl.semaphore_wait(barrier, 2 + 3 * sides)
    launch(0, 1, 0)
    eps = sensor(lambda p: state[0, p], work)
    eps_out[...] = eps
    around[1, 1] = eps
    for dx, dy in offsets:
        guarded(reachable(dx), lambda dx=dx, dy=dy: eps_copy(dx, dy).start())

    send_traces(0, 0)
    launch(0, 0, 0)

    def later_traces(v, carry):
        load(v).wait()
        for axis in (1, 0):
            send_traces(axis, v)
            launch(0, axis, v)
        return carry

    lax.fori_loop(1, count, later_traces, 0)

    lane = lax.broadcasted_iota(jnp.int32, (rows, lanes), 1)
    first, last = lane == 0, lane == lanes - 1

    def normal_gradient(v, carry):
        def body(q, carry):
            for j in range(5):
                pts = points(2, q, j)
                parts = fold([state[v, p] for p in pts])
                left, right = traces(parts)
                before = jnp.where(first, left, rolled(right, 1, 1))
                after = jnp.where(last, right, rolled(left, -1, 1))
                for p, value in zip(pts, slope(parts, before, after)):
                    grad[v, p] = value
            return carry

        lax.fori_loop(0, 5, body, 0)
        return carry

    lax.fori_loop(0, count, normal_gradient, 0)

    row = lax.broadcasted_iota(jnp.int32, (rows, lanes), 0)
    for dx, dy in offsets:
        guarded(reachable(-dx), lambda dx=dx, dy=dy: eps_copy(dx, dy).wait_recv())

    have_low = jnp.where(me_c > 0, spans, 0)
    have_high = jnp.where(me_c + 1 < chord_size, rows, rows - spans)
    low_s, high_s = masks[1]
    low_c, high_c = masks[0]
    column = []
    for x in range(3):
        mine, left, right = around[x, 1], around[x, 0], around[x, 2]
        column.append([
            jnp.where(low_s, rolled(left, 1 - spans, 0), rolled(mine, 1, 0)),
            mine,
            jnp.where(high_s, rolled(right, spans - 1, 0), rolled(mine, -1, 0)),
            jnp.where(low_s, rolled(left, 2 - spans, 0), rolled(right, spans - 2, 0)),
        ])
    closed_low = row < spans - have_low
    closed_high = row >= have_high
    neighbours = [[], [], [], []]
    for y in range(4):
        inner = column[1][y]
        below = jnp.where(low_c, rolled(column[0][y], spans, 0), rolled(inner, spans, 0))
        above = jnp.where(high_c, rolled(column[2][y], -spans, 0), rolled(inner, -spans, 0))
        beyond = jnp.where(
            low_c, rolled(column[0][y], 2 * spans, 0), rolled(column[2][y], -2 * spans, 0)
        )
        neighbours[0].append(jnp.where(closed_low, 0.0, below))
        neighbours[1].append(inner)
        neighbours[2].append(jnp.where(closed_high, 0.0, above))
        neighbours[3].append(beyond)
    corner = interpolate(neighbours, nu)
    near_weight = sum(float(LEFT[i] * HALF_LEFT[i] * (1.0 - NODES[i]) / 2.0) for i in range(5))
    far_weight = sum(float(LEFT[i] * HALF_LEFT[i] * (1.0 + NODES[i]) / 2.0) for i in range(5))
    for axis in range(2):
        low = masks[axis][0]
        sign = jnp.where(low, -1.0, 1.0)
        weight = {}
        for t in range(2):
            pair = []
            for o in (t, t + 1):
                if axis == 0:
                    pair += [jnp.where(low, neighbours[0][o], neighbours[2][o]), neighbours[3][o]]
                else:
                    pair += [jnp.where(low, neighbours[o][0], neighbours[o][2]), neighbours[o][3]]
            line = jnp.maximum(jnp.maximum(pair[0], pair[1]), jnp.maximum(pair[2], pair[3]))
            far = along_lanes(line)
            for z in range(2):
                if axis == 0:
                    near = jnp.where(low, corner[0, t, z], corner[1, t, z])
                else:
                    near = jnp.where(low, corner[t, 0, z], corner[t, 1, z])
                weight[t, z] = sign * (near_weight * near + far_weight * far[z])
        for m in range(5):
            ends = [LOWER[m] * weight[0, z] + UPPER[m] * weight[1, z] for z in range(2)]
            for c in range(5):
                beta[axis, 5 * m + c] = LOWER[c] * ends[0] + UPPER[c] * ends[1]

    for axis in (1, 0):

        def variable(v, carry):
            up, down = sends[1][2 * axis], sends[1][2 * axis + 1]
            low, high = masks[axis]
            step = spans if axis == 0 else 1

            def body(q, carry):
                for j in range(5):
                    pts = points(axis, q, j)
                    parts = fold([state[v, p] for p in pts])
                    left, right = traces(parts)
                    before = jnp.where(low, 0.0, rolled(right, step, 0))
                    after = jnp.where(high, 0.0, rolled(left, -step, 0))
                    if axis == 0:
                        before = jnp.where(closed_low, left, before)
                        after = jnp.where(closed_high, right, after)
                    gradient = slope(parts, before, after)
                    parts = fold([nu[p] * g for p, g in zip(pts, gradient)])
                    left, right = traces(parts)
                    store_pair(work, j, left, right, down, up, (v, 5 * q + j), *outer[axis])
                    before = jnp.where(low, 0.0, rolled(right, step, 0))
                    after = jnp.where(high, 0.0, rolled(left, -step, 0))
                    if axis == 0:
                        before = jnp.where(closed_low, -left, before)
                        after = jnp.where(closed_high, -right, after)
                    for p, value in zip(pts, slope(parts, before, after)):
                        if axis == 1:
                            acc[v, p] = value
                        else:
                            acc[v, p] += value
                return carry

            lax.fori_loop(0, 5, body, 0)
            launch(1, axis, v)
            return carry

        lax.fori_loop(0, count, variable, 0)

    for axis in range(2):
        low, high = masks[axis]

        def gains(q, carry):
            for j in range(5):
                f = 5 * q + j
                spread = []
                for i, p in enumerate(points(axis, q, j)):
                    lift = jnp.where(high, float(HALF_RIGHT[i]), 0.0)
                    spread.append(nu[p] * jnp.where(low, float(HALF_LEFT[i]), lift))
                parts = fold(spread)
                left, right = traces(parts)
                edge[axis, 2 * f] = left
                edge[axis, 2 * f + 1] = right
                for i, value in enumerate(slope(parts, None, None)):
                    gain[axis, 5 * f + i] = value
            return carry

        lax.fori_loop(0, 5, gains, 0)

    def normal(v, carry):
        def body(q, carry):
            for j in range(5):
                pts = points(2, q, j)
                parts = fold([nu[p] * grad[v, p] for p in pts])
                left, right = traces(parts)
                before = jnp.where(first, -left, rolled(right, 1, 1))
                after = jnp.where(last, -right, rolled(left, -1, 1))
                for p, value in zip(pts, slope(parts, before, after)):
                    acc[v, p] += value
            return carry

        lax.fori_loop(0, 5, body, 0)
        return carry

    lax.fori_loop(0, count, normal, 0)

    def arrived(axis, v):
        for k in (2 * axis, 2 * axis + 1):
            for stage in range(2):
                guarded(
                    reachable(-ways[k][0]),
                    lambda k=k, stage=stage: message(stage, k, v).wait_recv(),
                )

    for axis in (0, 1):

        def correct(v, carry):
            arrived(axis, v)
            up, down = ghosts[2 * axis], ghosts[2 * axis + 1]
            f_up, f_down = flux_ghosts[2 * axis], flux_ghosts[2 * axis + 1]
            faces = (faces_c, faces_s)[axis]
            low, high = masks[axis]
            rows_low, rows_high = outer[axis]
            step = spans if axis == 0 else 1
            opened = low | high
            if axis == 0:
                opened = opened & jnp.logical_not(closed_low | closed_high)

            def gather(q, carry):
                for j in range(5):
                    f = 5 * q + j
                    outside[f, rows_low] = up[v, f]
                    outside[f, rows_high] = down[v, f]
                    alpha[f, rows_low] = f_up[v, f]
                    alpha[f, rows_high] = f_down[v, f]
                return carry

            lax.fori_loop(0, 5, gather, 0)

            def body(q, carry):
                for j in range(5):
                    f = 5 * q + j
                    ghost = jnp.where(opened, outside[f], 0.0)
                    flux = jnp.where(opened, alpha[f] + beta[axis, f] * faces[v, f], 0.0)
                    before = jnp.where(low, flux, rolled(edge[axis, 2 * f + 1] * ghost, step, 0))
                    after = jnp.where(high, flux, rolled(edge[axis, 2 * f] * ghost, -step, 0))
                    h = [float(x) for x in HALF_LEFT]
                    diff, both = before - after, before + after
                    even = [0.5 * (h[i] + h[4 - i]) * diff for i in range(3)]
                    odd = [0.5 * (h[i] - h[4 - i]) * both for i in range(2)]
                    lifts = [
                        even[0] + odd[0], even[1] + odd[1], even[2],
                        even[1] - odd[1], even[0] - odd[0],
                    ]
                    for i, p in enumerate(points(axis, q, j)):
                        acc[v, p] += gain[axis, 5 * f + i] * ghost + lifts[i]
                return carry

            lax.fori_loop(0, 5, body, 0)
            return carry

        lax.fori_loop(0, count, correct, 0)

    for dx, dy in offsets:
        guarded(reachable(dx), lambda dx=dx, dy=dy: eps_copy(dx, dy).wait_send())
    for stage in range(2):
        for k in range(4):
            for v in range(count):
                guarded(
                    reachable(ways[k][0]),
                    lambda stage=stage, k=k, v=v: message(stage, k, v).wait_send(),
                )


def shards(state):
    count, npts, chords, spans, lanes = state.shape
    rows = chords * spans
    flat = state.reshape(count, npts, rows, lanes)
    f32 = jnp.float32
    sizes = (lax.axis_size("chord"), lax.axis_size("span"))

    def message(n, k):
        return (n, 25, spans if k < 2 else chords, lanes)

    def full(*shape):
        return jax.ShapeDtypeStruct(shape, f32)

    vmem = pl.BlockSpec(memory_space=pltpu.VMEM)
    nu, residual = pl.pallas_call(
        functools.partial(local_kernel, sizes, count, chords, spans),
        in_specs=[pl.BlockSpec(memory_space=pltpu.HBM)],
        out_specs=[vmem, vmem],
        out_shape=[full(npts, rows, lanes), full(count, npts, rows, lanes)],
        scratch_shapes=[
            pltpu.VMEM(shape, f32)
            for shape in [
                (count, npts, rows, lanes),
                (count, npts, rows, lanes),
                (3, 3, rows, lanes),
                (npts, rows, lanes),
                (rows, lanes),
                (count, 25, rows, lanes),
                (count, 25, rows, lanes),
                (2, npts, rows, lanes),
                (2, 50, rows, lanes),
                (2, 25, rows, lanes),
                (25, rows, lanes),
                (25, rows, lanes),
            ]
            + [message(count, k) for k in range(4)] * 4
        ]
        + [
            pltpu.SemaphoreType.DMA((count,)),
            pltpu.SemaphoreType.DMA((9,)),
            pltpu.SemaphoreType.DMA((9,)),
            pltpu.SemaphoreType.DMA((2, 4, count)),
            pltpu.SemaphoreType.DMA((2, 4, count)),
        ],
        compiler_params=pltpu.CompilerParams(
            collective_id=0, has_side_effects=True, vmem_limit_bytes=VMEM_BYTES
        ),
    )(flat)
    return residual.reshape(state.shape), nu.reshape(npts, chords, spans, lanes)


def solution(mesh):
    in_specs = (P(None, None, "chord", "span", None),)
    out_specs = (P(None, None, "chord", "span", None), P(None, "chord", "span", None))
    return jax.shard_map(shards, mesh=mesh, in_specs=in_specs, out_specs=out_specs, check_vma=False)
```

```python
import functools
import math

import jax
import jax.numpy as jnp
import numpy as np
from jax import lax
from jax.experimental import pallas as pl
from jax.experimental.pallas import tpu as pltpu
from jax.sharding import PartitionSpec as P

VMEM_BYTES = 52_500_000
EPS_SCALE = 0.01
SENSOR_CENTRE = -3.0
SENSOR_WIDTH = 1.5
RATIO_FLOOR = 1e-06
ENERGY_EPS = 1e-06
GAUSS_NODES = [-0.906179845938664, -0.5384693101056831, 0.0, 0.5384693101056831, 0.906179845938664]
GAUSS_WEIGHTS = [
    0.2369268850561891,
    0.4786286704993665,
    0.5688888888888889,
    0.4786286704993665,
    0.2369268850561891,
]


def legendre_values(points):
    values = [np.ones(points.shape), np.array(points)]
    for order in range(1, 5):
        values.append(
            ((2 * order + 1) * points * values[order] - order * values[order - 1]) / (order + 1)
        )
    return values


def line_tables():
    line_nodes = np.array(GAUSS_NODES)
    quadrature_weights = np.array(GAUSS_WEIGHTS)
    barycentric = np.array(
        [
            1.0 / np.prod([line_nodes[j] - line_nodes[k] for k in range(5) if k != j])
            for j in range(5)
        ]
    )
    derivative = np.zeros((5, 5))
    for i in range(5):
        for j in range(5):
            if i != j:
                derivative[i, j] = barycentric[j] / barycentric[i] / (line_nodes[i] - line_nodes[j])
        derivative[i, i] = -np.sum(derivative[i])
    left_values = np.ones(5)
    right_values = np.ones(5)
    for j in range(5):
        for k in range(5):
            if k != j:
                left_values[j] *= (-1.0 - line_nodes[k]) / (line_nodes[j] - line_nodes[k])
                right_values[j] *= (1.0 - line_nodes[k]) / (line_nodes[j] - line_nodes[k])
    legendre = legendre_values(line_nodes)
    fourth_slope = 7.0 * legendre[3] + 3.0 * legendre[1]
    fifth_slope = 9.0 * legendre[4] + 5.0 * legendre[2] + legendre[0]
    left_corr = 0.5 * (fourth_slope - fifth_slope)
    right_corr = 0.5 * (fourth_slope + fifth_slope)
    modal = np.zeros((5, 5))
    for k in range(5):
        modal[k, :] = quadrature_weights * math.sqrt((2 * k + 1) / 2.0) * legendre[k]
    return (line_nodes, derivative, left_values, right_values, left_corr, right_corr, modal)


NODES, DERIV, LEFT, RIGHT, LIFT_LEFT, LIFT_RIGHT, MODAL = line_tables()
HALF_LEFT = 0.5 * LIFT_LEFT
HALF_RIGHT = 0.5 * LIFT_RIGHT


def fold(u):
    return (u[0] + u[4], u[1] + u[3], u[2], u[0] - u[4], u[1] - u[3])


def traces(parts):
    s0, s1, mid, d0, d1 = parts
    r = [float(x) for x in RIGHT]
    even = 0.5 * (r[0] + r[4]) * s0 + 0.5 * (r[1] + r[3]) * s1 + r[2] * mid
    odd = 0.5 * (r[0] - r[4]) * d0 + 0.5 * (r[1] - r[3]) * d1
    return even - odd, even + odd


def slope(parts, before, after):
    s0, s1, mid, d0, d1 = parts
    h = [float(x) for x in HALF_LEFT]
    r = [float(x) for x in RIGHT]
    if before is not None:
        diff, both = before - after, before + after
    even, odd = [], []
    for i in range(3):
        lift = 0.5 * (h[i] + h[4 - i])
        value = (
            float(0.5 * (DERIV[i, 0] - DERIV[i, 4]) + lift * (r[0] - r[4])) * d0
            + float(0.5 * (DERIV[i, 1] - DERIV[i, 3]) + lift * (r[1] - r[3])) * d1
        )
        even.append(value if before is None else value + lift * diff)
    for i in range(2):
        lift = 0.5 * (h[i] - h[4 - i])
        value = (
            float(0.5 * (DERIV[i, 0] + DERIV[i, 4]) - lift * (r[0] + r[4])) * s0
            + float(0.5 * (DERIV[i, 1] + DERIV[i, 3]) - lift * (r[1] + r[3])) * s1
            + float(DERIV[i, 2] - 2.0 * lift * r[2]) * mid
        )
        odd.append(value if before is None else value + lift * both)
    return [even[0] + odd[0], even[1] + odd[1], even[2], even[1] - odd[1], even[0] - odd[0]]


def points(axis, q, j):
    if axis == 0:
        return [25 * i + 5 * q + j for i in range(5)]
    if axis == 1:
        return [25 * q + 5 * i + j for i in range(5)]
    return [25 * q + 5 * j + i for i in range(5)]


def modal_line(u):
    s0, s1, mid, d0, d1 = fold(u)
    out = []
    for k in range(5):
        m = [float(x) for x in MODAL[k]]
        out.append(m[0] * s0 + m[1] * s1 + m[2] * mid if k % 2 == 0 else m[0] * d0 + m[1] * d1)
    return out


def sensor(load, work):
    def first(q, carry):
        for j in range(5):
            pts = points(0, q, j)
            for i, value in zip(pts, modal_line([load(p) for p in pts])):
                work[i] = value
        return carry

    lax.fori_loop(0, 5, first, 0)

    def second(q, carry):
        total, high = carry
        plane = {}
        for c in range(5):
            for b, value in enumerate(modal_line([work[25 * q + 5 * b + c] for b in range(5)])):
                plane[b, c] = value
        low = jnp.zeros_like(total)
        edge = jnp.zeros_like(total)
        for b in range(5):
            line = modal_line([plane[b, c] for c in range(5)])
            squares = [x * x for x in line]
            if b < 4:
                low = low + ((squares[0] + squares[1]) + (squares[2] + squares[3]))
                edge = edge + squares[4]
            else:
                edge = edge + ((squares[0] + squares[1]) + (squares[2] + squares[3])) + squares[4]
        plane_total = low + edge
        return total + plane_total, high + jnp.where(q == 4, plane_total, edge)

    zero = jnp.zeros(work.shape[1:], jnp.float32)
    total, high = lax.fori_loop(0, 5, second, (zero, zero))
    level = jnp.log(jnp.maximum(high / (total + ENERGY_EPS), RATIO_FLOOR)) * (1.0 / math.log(10.0))
    ramp = jnp.clip((level - SENSOR_CENTRE) / SENSOR_WIDTH, -1.0, 1.0)
    return EPS_SCALE * 0.5 * (1.0 + jnp.sin(0.5 * math.pi * ramp))


def rolled(value, shift, axis):
    size = value.shape[axis]
    return pltpu.roll(value, shift % size, axis)


LOWER = [float((1.0 - x) / 2.0) for x in NODES]
UPPER = [float((1.0 + x) / 2.0) for x in NODES]


def along_lanes(line):
    lanes = line.shape[1]
    lane = lax.broadcasted_iota(jnp.int32, line.shape, 1)
    before = jnp.where(lane == 0, 0.0, rolled(line, 1, 1))
    after = jnp.where(lane == lanes - 1, 0.0, rolled(line, -1, 1))
    return jnp.maximum(line, before), jnp.maximum(line, after)


def interpolate(neighbours, nu):
    corner = {}
    for x in range(2):
        for y in range(2):
            line = jnp.maximum(
                jnp.maximum(neighbours[x][y], neighbours[x + 1][y]),
                jnp.maximum(neighbours[x][y + 1], neighbours[x + 1][y + 1]),
            )
            corner[x, y, 0], corner[x, y, 1] = along_lanes(line)
    lower, upper = LOWER, UPPER
    for a in range(5):
        face = {
            (y, z): lower[a] * corner[0, y, z] + upper[a] * corner[1, y, z]
            for y in range(2)
            for z in range(2)
        }
        for b in range(5):
            edge = [lower[b] * face[0, z] + upper[b] * face[1, z] for z in range(2)]
            for c in range(5):
                nu[25 * a + 5 * b + c] = lower[c] * edge[0] + upper[c] * edge[1]
    return corner


def row_masks(axis, chords, spans, lanes):
    row = lax.broadcasted_iota(jnp.int32, (chords * spans, lanes), 0)
    if axis == 0:
        return row < spans, row >= (chords - 1) * spans
    place = row % spans
    return place == 0, place == spans - 1


def outer_rows(axis, chords, spans, last):
    if axis == 0:
        return pl.ds((chords - 1) * spans if last else 0, spans)
    return pl.ds(spans - 1 if last else 0, chords, spans)


def store_pair(work, slot, left, right, down, up, index, rows_low, rows_high):
    work[2 * slot] = left
    work[2 * slot + 1] = right
    down[index] = work[2 * slot, rows_low]
    up[index] = work[2 * slot + 1, rows_high]


def local_kernel(sizes, count, chords, spans, *refs):
    state_hbm = refs[0]
    nu, acc = refs[1:3]
    (
        state, grad, around, work, eps_out, faces_c, faces_s, gain, edge, beta, outside, alpha,
        t0, t1, t2, t3, f0, f1, f2, f3,
    ) = refs[3:23]
    ghosts, flux_ghosts = refs[23:27], refs[27:31]
    load_sem, eps_send, eps_recv, send_sem, recv_sem = refs[31:]
    sends = ((t0, t1, t2, t3), (f0, f1, f2, f3))
    lands = (ghosts, flux_ghosts)
    rows, lanes = nu.shape[1:]
    chord_size, span_size = sizes
    me_c, me_s = lax.axis_index("chord"), lax.axis_index("span")
    mesh_id = pl.DeviceIdType.MESH

    def load(v):
        return pltpu.make_async_copy(state_hbm.at[v], state.at[v], load_sem.at[v])

    for v in range(count):
        load(v).start()

    def reachable(dx):
        if dx == 0:
            return None
        return me_c + 1 < chord_size if dx == 1 else me_c > 0

    def guarded(cond, run):
        if cond is None:
            run()
        else:
            pl.when(cond)(run)

    def partner(dx, dy):
        return (me_c + dx, lax.rem(me_s + dy + span_size, span_size))

    offsets = [(dx, dy) for dx in (0, -1, 1) for dy in (-1, 0, 1) if (dx, dy) != (0, 0)]
    barrier = pltpu.get_barrier_semaphore()
    for dx, dy in offsets:

        def greet(dx=dx, dy=dy):
            pl.semaphore_signal(barrier, inc=1, device_id=partner(dx, dy), device_id_type=mesh_id)

        guarded(reachable(dx), greet)

    def eps_copy(dx, dy):
        slot = 3 * (dx + 1) + dy + 1
        return pltpu.make_async_remote_copy(
            src_ref=eps_out, dst_ref=around.at[1 - dx, 1 - dy],
            send_sem=eps_send.at[slot], recv_sem=eps_recv.at[8 - slot],
            device_id=partner(dx, dy), device_id_type=mesh_id,
        )

    ways = ((1, 0), (-1, 0), (0, 1), (0, -1))

    def message(stage, k, v):
        dx, dy = ways[k]
        return pltpu.make_async_remote_copy(
            src_ref=sends[stage][k].at[v], dst_ref=lands[stage][k].at[v],
            send_sem=send_sem.at[stage, k, v], recv_sem=recv_sem.at[stage, k, v],
            device_id=partner(dx, dy), device_id_type=mesh_id,
        )

    def launch(stage, axis, v):
        for k in (2 * axis, 2 * axis + 1):
            guarded(reachable(ways[k][0]), lambda k=k: message(stage, k, v).start())

    masks = [row_masks(axis, chords, spans, lanes) for axis in range(2)]
    outer = [[outer_rows(axis, chords, spans, last) for last in (False, True)] for axis in range(2)]

    def send_traces(axis, v):
        up, down = sends[0][2 * axis], sends[0][2 * axis + 1]
        faces = (faces_c, faces_s)[axis]

        def body(q, carry):
            for j in range(5):
                left, right = traces(fold([state[v, p] for p in points(axis, q, j)]))
                faces[v, 5 * q + j] = jnp.where(masks[axis][0], left, right)
                store_pair(work, j, left, right, down, up, (v, 5 * q + j), *outer[axis])
            return carry

        lax.fori_loop(0, 5, body, 0)

    load(0).wait()
    send_traces(1, 0)
    sides = jnp.where(me_c > 0, 1, 0) + jnp.where(me_c + 1 < chord_size, 1, 0)
    pl.semaphore_wait(barrier, 2 + 3 * sides)
    launch(0, 1, 0)
    eps = sensor(lambda p: state[0, p], work)
    eps_out[...] = eps
    around[1, 1] = eps
    for dx, dy in offsets:
        guarded(reachable(dx), lambda dx=dx, dy=dy: eps_copy(dx, dy).start())

    send_traces(0, 0)
    launch(0, 0, 0)

    def later_traces(v, carry):
        load(v).wait()
        for axis in (1, 0):
            send_traces(axis, v)
            launch(0, axis, v)
        return carry

    lax.fori_loop(1, count, later_traces, 0)

    lane = lax.broadcasted_iota(jnp.int32, (rows, lanes), 1)
    first, last = lane == 0, lane == lanes - 1

    def normal_gradient(v, carry):
        def body(q, carry):
            for j in range(5):
                pts = points(2, q, j)
                parts = fold([state[v, p] for p in pts])
                left, right = traces(parts)
                before = jnp.where(first, left, rolled(right, 1, 1))
                after = jnp.where(last, right, rolled(left, -1, 1))
                for p, value in zip(pts, slope(parts, before, after)):
                    grad[v, p] = value
            return carry

        lax.fori_loop(0, 5, body, 0, unroll=True)
        return carry

    lax.fori_loop(0, count, normal_gradient, 0)

    row = lax.broadcasted_iota(jnp.int32, (rows, lanes), 0)
    for dx, dy in offsets:
        guarded(reachable(-dx), lambda dx=dx, dy=dy: eps_copy(dx, dy).wait_recv())

    have_low = jnp.where(me_c > 0, spans, 0)
    have_high = jnp.where(me_c + 1 < chord_size, rows, rows - spans)
    low_s, high_s = masks[1]
    low_c, high_c = masks[0]
    column = []
    for x in range(3):
        mine, left, right = around[x, 1], around[x, 0], around[x, 2]
        column.append([
            jnp.where(low_s, rolled(left, 1 - spans, 0), rolled(mine, 1, 0)),
            mine,
            jnp.where(high_s, rolled(right, spans - 1, 0), rolled(mine, -1, 0)),
            jnp.where(low_s, rolled(left, 2 - spans, 0), rolled(right, spans - 2, 0)),
        ])
    closed_low = row < spans - have_low
    closed_high = row >= have_high
    neighbours = [[], [], [], []]
    for y in range(4):
        inner = column[1][y]
        below = jnp.where(low_c, rolled(column[0][y], spans, 0), rolled(inner, spans, 0))
        above = jnp.where(high_c, rolled(column[2][y], -spans, 0), rolled(inner, -spans, 0))
        beyond = jnp.where(
            low_c, rolled(column[0][y], 2 * spans, 0), rolled(column[2][y], -2 * spans, 0)
        )
        neighbours[0].append(jnp.where(closed_low, 0.0, below))
        neighbours[1].append(inner)
        neighbours[2].append(jnp.where(closed_high, 0.0, above))
        neighbours[3].append(beyond)
    corner = interpolate(neighbours, nu)
    near_weight = sum(float(LEFT[i] * HALF_LEFT[i] * (1.0 - NODES[i]) / 2.0) for i in range(5))
    far_weight = sum(float(LEFT[i] * HALF_LEFT[i] * (1.0 + NODES[i]) / 2.0) for i in range(5))
    for axis in range(2):
        low = masks[axis][0]
        sign = jnp.where(low, -1.0, 1.0)
        weight = {}
        for t in range(2):
            pair = []
            for o in (t, t + 1):
                if axis == 0:
                    pair += [jnp.where(low, neighbours[0][o], neighbours[2][o]), neighbours[3][o]]
                else:
                    pair += [jnp.where(low, neighbours[o][0], neighbours[o][2]), neighbours[o][3]]
            line = jnp.maximum(jnp.maximum(pair[0], pair[1]), jnp.maximum(pair[2], pair[3]))
            far = along_lanes(line)
            for z in range(2):
                if axis == 0:
                    near = jnp.where(low, corner[0, t, z], corner[1, t, z])
                else:
                    near = jnp.where(low, corner[t, 0, z], corner[t, 1, z])
                weight[t, z] = sign * (near_weight * near + far_weight * far[z])
        for m in range(5):
            ends = [LOWER[m] * weight[0, z] + UPPER[m] * weight[1, z] for z in range(2)]
            for c in range(5):
                beta[axis, 5 * m + c] = LOWER[c] * ends[0] + UPPER[c] * ends[1]

    for axis in (1, 0):

        def variable(v, carry):
            up, down = sends[1][2 * axis], sends[1][2 * axis + 1]
            low, high = masks[axis]
            step = spans if axis == 0 else 1

            def body(q, carry):
                for j in range(5):
                    pts = points(axis, q, j)
                    parts = fold([state[v, p] for p in pts])
                    left, right = traces(parts)
                    before = jnp.where(low, 0.0, rolled(right, step, 0))
                    after = jnp.where(high, 0.0, rolled(left, -step, 0))
                    if axis == 0:
                        before = jnp.where(closed_low, left, before)
                        after = jnp.where(closed_high, right, after)
                    gradient = slope(parts, before, after)
                    parts = fold([nu[p] * g for p, g in zip(pts, gradient)])
                    left, right = traces(parts)
                    store_pair(work, j, left, right, down, up, (v, 5 * q + j), *outer[axis])
                    before = jnp.where(low, 0.0, rolled(right, step, 0))
                    after = jnp.where(high, 0.0, rolled(left, -step, 0))
                    if axis == 0:
                        before = jnp.where(closed_low, -left, before)
                        after = jnp.where(closed_high, -right, after)
                    for p, value in zip(pts, slope(parts, before, after)):
                        if axis == 1:
                            acc[v, p] = value
                        else:
                            acc[v, p] += value
                return carry

            lax.fori_loop(0, 5, body, 0, unroll=True)
            launch(1, axis, v)
            return carry

        lax.fori_loop(0, count, variable, 0)

    for axis in range(2):
        low, high = masks[axis]

        def gains(q, carry):
            for j in range(5):
                f = 5 * q + j
                spread = []
                for i, p in enumerate(points(axis, q, j)):
                    lift = jnp.where(high, float(HALF_RIGHT[i]), 0.0)
                    spread.append(nu[p] * jnp.where(low, float(HALF_LEFT[i]), lift))
                parts = fold(spread)
                left, right = traces(parts)
                edge[axis, 2 * f] = left
                edge[axis, 2 * f + 1] = right
                for i, value in enumerate(slope(parts, None, None)):
                    gain[axis, 5 * f + i] = value
            return carry

        lax.fori_loop(0, 5, gains, 0)

    def normal(v, carry):
        def body(q, carry):
            for j in range(5):
                pts = points(2, q, j)
                parts = fold([nu[p] * grad[v, p] for p in pts])
                left, right = traces(parts)
                before = jnp.where(first, -left, rolled(right, 1, 1))
                after = jnp.where(last, -right, rolled(left, -1, 1))
                for p, value in zip(pts, slope(parts, before, after)):
                    acc[v, p] += value
            return carry

        lax.fori_loop(0, 5, body, 0, unroll=True)
        return carry

    lax.fori_loop(0, count, normal, 0)

    def arrived(axis, v):
        for k in (2 * axis, 2 * axis + 1):
            for stage in range(2):
                guarded(
                    reachable(-ways[k][0]),
                    lambda k=k, stage=stage: message(stage, k, v).wait_recv(),
                )

    for axis in (0, 1):

        def correct(v, carry):
            arrived(axis, v)
            up, down = ghosts[2 * axis], ghosts[2 * axis + 1]
            f_up, f_down = flux_ghosts[2 * axis], flux_ghosts[2 * axis + 1]
            faces = (faces_c, faces_s)[axis]
            low, high = masks[axis]
            rows_low, rows_high = outer[axis]
            step = spans if axis == 0 else 1
            opened = low | high
            if axis == 0:
                opened = opened & jnp.logical_not(closed_low | closed_high)

            def gather(q, carry):
                for j in range(5):
                    f = 5 * q + j
                    outside[f, rows_low] = up[v, f]
                    outside[f, rows_high] = down[v, f]
                    alpha[f, rows_low] = f_up[v, f]
                    alpha[f, rows_high] = f_down[v, f]
                return carry

            lax.fori_loop(0, 5, gather, 0)

            def body(q, carry):
                for j in range(5):
                    f = 5 * q + j
                    ghost = jnp.where(opened, outside[f], 0.0)
                    flux = jnp.where(opened, alpha[f] + beta[axis, f] * faces[v, f], 0.0)
                    before = jnp.where(low, flux, rolled(edge[axis, 2 * f + 1] * ghost, step, 0))
                    after = jnp.where(high, flux, rolled(edge[axis, 2 * f] * ghost, -step, 0))
                    h = [float(x) for x in HALF_LEFT]
                    diff, both = before - after, before + after
                    even = [0.5 * (h[i] + h[4 - i]) * diff for i in range(3)]
                    odd = [0.5 * (h[i] - h[4 - i]) * both for i in range(2)]
                    lifts = [
                        even[0] + odd[0], even[1] + odd[1], even[2],
                        even[1] - odd[1], even[0] - odd[0],
                    ]
                    for i, p in enumerate(points(axis, q, j)):
                        acc[v, p] += gain[axis, 5 * f + i] * ghost + lifts[i]
                return carry

            lax.fori_loop(0, 5, body, 0, unroll=True)
            return carry

        lax.fori_loop(0, count, correct, 0)

    for dx, dy in offsets:
        guarded(reachable(dx), lambda dx=dx, dy=dy: eps_copy(dx, dy).wait_send())
    for stage in range(2):
        for k in range(4):
            for v in range(count):
                guarded(
                    reachable(ways[k][0]),
                    lambda stage=stage, k=k, v=v: message(stage, k, v).wait_send(),
                )


def shards(state):
    count, npts, chords, spans, lanes = state.shape
    rows = chords * spans
    flat = state.reshape(count, npts, rows, lanes)
    f32 = jnp.float32
    sizes = (lax.axis_size("chord"), lax.axis_size("span"))

    def message(n, k):
        return (n, 25, spans if k < 2 else chords, lanes)

    def full(*shape):
        return jax.ShapeDtypeStruct(shape, f32)

    vmem = pl.BlockSpec(memory_space=pltpu.VMEM)
    nu, residual = pl.pallas_call(
        functools.partial(local_kernel, sizes, count, chords, spans),
        in_specs=[pl.BlockSpec(memory_space=pltpu.HBM)],
        out_specs=[vmem, vmem],
        out_shape=[full(npts, rows, lanes), full(count, npts, rows, lanes)],
        scratch_shapes=[
            pltpu.VMEM(shape, f32)
            for shape in [
                (count, npts, rows, lanes),
                (count, npts, rows, lanes),
                (3, 3, rows, lanes),
                (npts, rows, lanes),
                (rows, lanes),
                (count, 25, rows, lanes),
                (count, 25, rows, lanes),
                (2, npts, rows, lanes),
                (2, 50, rows, lanes),
                (2, 25, rows, lanes),
                (25, rows, lanes),
                (25, rows, lanes),
            ]
            + [message(count, k) for k in range(4)] * 4
        ]
        + [
            pltpu.SemaphoreType.DMA((count,)),
            pltpu.SemaphoreType.DMA((9,)),
            pltpu.SemaphoreType.DMA((9,)),
            pltpu.SemaphoreType.DMA((2, 4, count)),
            pltpu.SemaphoreType.DMA((2, 4, count)),
        ],
        compiler_params=pltpu.CompilerParams(
            collective_id=0, has_side_effects=True, vmem_limit_bytes=VMEM_BYTES
        ),
    )(flat)
    return residual.reshape(state.shape), nu.reshape(npts, chords, spans, lanes)


def solution(mesh):
    in_specs = (P(None, None, "chord", "span", None),)
    out_specs = (P(None, None, "chord", "span", None), P(None, "chord", "span", None))
    return jax.shard_map(shards, mesh=mesh, in_specs=in_specs, out_specs=out_specs, check_vma=False)
```
